64 devices in a mesh: data: 4 (over x, y), expert: 16 (over z, core).
Axes of the slice: x: 2, y: 2, z: 8, core: 2. Of those that a mesh axis runs over, the one named last changes fastest.
The devices are a block of a 4x4x8 slice.
Arguments:
- tokens: bfloat16 [8192, 1024], P(('data', 'expert')), parts along dimension 0
- expert_ids: int32 [8192, 8], P(('data', 'expert')), parts along dimension 0
- gate_wts: float32 [8192, 8], P(('data', 'expert')), parts along dimension 0
- dev_slot: int32 [8192, 8], P(('data', 'expert')), parts along dimension 0
- exp_slot: int32 [8192, 8], P(('data', 'expert')), parts along dimension 0
- w_gate: bfloat16 [32, 1024, 512], P('expert')
- w_up: bfloat16 [32, 1024, 512], P('expert')
- w_down: bfloat16 [32, 512, 1024], P('expert')
Outputs:
- output: bfloat16 [8192, 1024], P(('data', 'expert')), parts along dimension 0
There are 4 independent parts. The reference program is written for one: setup_inputs(seed, part) draws one part's arguments, and reference() takes and returns one part's arrays. A program takes and returns all parts, laid end to end along the dimension named above; an argument that names none is the same for every part.
All inputs are finite; a program needn't handle non-finite values.
Results may differ from the reference program's by a relative error of at most 0.00784104.
Values are sent between devices in bfloat16 or wider.
A program may use at most 768 MiB of HBM per device.

```python
import jax
import jax.numpy as jnp
from jax import lax

TOK_DEV = 128
GROUP_SIZE = 16
D_MODEL = 1024
D_FF = 512
N_EXPERTS = 32
TOP_K = 8

TOKENS = TOK_DEV * GROUP_SIZE
E_LOCAL = N_EXPERTS // GROUP_SIZE
DEV_CAP = min(TOK_DEV, 8 * ((3 * TOK_DEV * TOP_K + 16 * GROUP_SIZE - 1) // (16 * GROUP_SIZE)))
EXP_CAP = 8 * ((TOKENS * TOP_K + 4 * N_EXPERTS - 1) // (4 * N_EXPERTS))
HOT_ROWS = (EXP_CAP + GROUP_SIZE - 1) // GROUP_SIZE
N_ROWS = GROUP_SIZE * DEV_CAP


def draw_routing(key):
    noise_key, skew_key = jax.random.split(key)
    noise_int = jax.random.randint(noise_key, (TOKENS, N_EXPERTS), 0, 1024)
    skew_bias = jax.random.randint(skew_key, (N_EXPERTS,), 0, 512)
    tok_pos = jnp.arange(TOKENS) % TOK_DEV
    src_dev = jnp.arange(TOKENS) // TOK_DEV
    ex_range = jnp.arange(N_EXPERTS)
    fwd_expert = ((src_dev + 1) % GROUP_SIZE) * E_LOCAL + tok_pos % E_LOCAL
    forced = (ex_range[None, :] == fwd_expert[:, None]) & (tok_pos[:, None] < DEV_CAP)
    hot_pick = (ex_range[None, :] == 0) & (tok_pos[:, None] < HOT_ROWS)
    score_int = noise_int + skew_bias[None, :] + 4096 * (forced | hot_pick).astype(jnp.int32)
    ranked = score_int * N_EXPERTS + ex_range[None, :]
    expert_ids = lax.top_k(ranked, TOP_K)[1].astype(jnp.int32)
    owner_dev = expert_ids // E_LOCAL
    dev_range = jnp.arange(GROUP_SIZE)

    def source_rank(src_owner):
        touch_dev = jnp.any(src_owner[:, :, None] == dev_range[None, None, :], axis=1).astype(jnp.int32)
        before = jnp.cumsum(touch_dev, axis=0) - touch_dev
        return jnp.take_along_axis(before, src_owner, axis=1)

    dev_rank = lax.map(source_rank, owner_dev.reshape(GROUP_SIZE, TOK_DEV, TOP_K)).reshape(TOKENS, TOP_K)
    dev_keep = dev_rank < DEV_CAP
    exp_loads = jnp.zeros((TOKENS, N_EXPERTS), jnp.int32).at[jnp.arange(TOKENS)[:, None], expert_ids].add(dev_keep.astype(jnp.int32))
    exp_before = jnp.cumsum(exp_loads, axis=0) - exp_loads
    exp_rank = jnp.take_along_axis(exp_before, expert_ids, axis=1)
    kept_choice = dev_keep & (exp_rank < EXP_CAP)
    dev_slot = jnp.where(kept_choice, dev_rank, -1).astype(jnp.int32)
    exp_slot = jnp.where(kept_choice, exp_rank, -1).astype(jnp.int32)
    return expert_ids, dev_slot, exp_slot


def setup_inputs(seed: int = 0, part: int = 0) -> dict:
    base_key = jax.random.key(seed)
    part_key = jax.random.fold_in(base_key, part)
    tok_key, gate_key, route_key = jax.random.split(part_key, 3)
    wg_key, wu_key, wd_key = jax.random.split(jax.random.fold_in(base_key, 1000), 3)
    tokens = jax.random.normal(tok_key, (TOKENS, D_MODEL), jnp.float32).astype(jnp.bfloat16)
    gate_wts = (0.5 + jax.random.uniform(gate_key, (TOKENS, TOP_K), jnp.float32)) * TOP_K ** -0.5
    expert_ids, dev_slot, exp_slot = draw_routing(route_key)
    w_gate = (jax.random.normal(wg_key, (N_EXPERTS, D_MODEL, D_FF), jnp.float32) * D_MODEL ** -0.5).astype(jnp.bfloat16)
    w_up = (jax.random.normal(wu_key, (N_EXPERTS, D_MODEL, D_FF), jnp.float32) * D_MODEL ** -0.5).astype(jnp.bfloat16)
    w_down = (jax.random.normal(wd_key, (N_EXPERTS, D_FF, D_MODEL), jnp.float32) * D_FF ** -0.5).astype(jnp.bfloat16)
    return {"tokens": tokens, "expert_ids": expert_ids, "gate_wts": gate_wts, "dev_slot": dev_slot, "exp_slot": exp_slot, "w_gate": w_gate, "w_up": w_up, "w_down": w_down}


def reference(tokens, expert_ids, gate_wts, dev_slot, exp_slot, w_gate, w_up, w_down):
    owner_dev = expert_ids // E_LOCAL
    local_ex = expert_ids % E_LOCAL
    src_dev = (jnp.arange(TOKENS) // TOK_DEV)[:, None]
    row_idx = src_dev * DEV_CAP + dev_slot
    gate_bf = gate_wts.astype(jnp.bfloat16).astype(jnp.float32)
    tok_f32 = tokens.astype(jnp.float32)
    gate_all = w_gate.reshape(GROUP_SIZE, E_LOCAL, D_MODEL, D_FF)
    up_all = w_up.reshape(GROUP_SIZE, E_LOCAL, D_MODEL, D_FF)
    down_all = w_down.reshape(GROUP_SIZE, E_LOCAL, D_FF, D_MODEL)

    def device_step(out_acc, dest_dev):
        on_dest = (owner_dev == dest_dev) & (dev_slot >= 0)
        tok_row = jnp.max(jnp.where(on_dest, row_idx, -1), axis=1)
        tok_dest = jnp.where(tok_row >= 0, tok_row, N_ROWS)
        recv_rows = jnp.zeros((N_ROWS, D_MODEL), jnp.float32).at[tok_dest].add(tok_f32, mode="drop")
        recv_rows = recv_rows.astype(jnp.bfloat16).astype(jnp.float32)
        choice_ok = on_dest & (exp_slot >= 0)
        flat_ex = jnp.where(choice_ok, local_ex, E_LOCAL).reshape(-1)
        flat_pos = jnp.where(choice_ok, exp_slot, 0).reshape(-1)
        row_of = jnp.full((E_LOCAL, EXP_CAP), -1, jnp.int32).at[flat_ex, flat_pos].max(row_idx.reshape(-1), mode="drop")
        gate_of = jnp.zeros((E_LOCAL, EXP_CAP), jnp.float32).at[flat_ex, flat_pos].add(gate_bf.reshape(-1), mode="drop")
        filled = row_of >= 0
        exp_in = jnp.where(filled[:, :, None], recv_rows[jnp.maximum(row_of, 0)], 0.0)
        w_one = gate_all[dest_dev].astype(jnp.float32)
        w_two = up_all[dest_dev].astype(jnp.float32)
        w_three = down_all[dest_dev].astype(jnp.float32)
        hid_gate = jnp.einsum("esd,edf->esf", exp_in, w_one)
        hid_up = jnp.einsum("esd,edf->esf", exp_in, w_two)
        hidden = (jax.nn.silu(hid_gate) * hid_up).astype(jnp.bfloat16).astype(jnp.float32)
        exp_out = jnp.einsum("esf,efd->esd", hidden, w_three).astype(jnp.bfloat16).astype(jnp.float32)
        back_dest = jnp.where(filled, row_of, N_ROWS).reshape(-1)
        weighted = (gate_of[:, :, None] * exp_out).reshape(-1, D_MODEL)
        z_rows = jnp.zeros((N_ROWS, D_MODEL), jnp.float32).at[back_dest].add(weighted, mode="drop")
        z_rows = z_rows.astype(jnp.bfloat16).astype(jnp.float32)
        back_rows = jnp.where((tok_row >= 0)[:, None], z_rows[jnp.maximum(tok_row, 0)], 0.0)
        return out_acc + back_rows, None

    out_acc, unused_stack = lax.scan(device_step, jnp.zeros((TOKENS, D_MODEL), jnp.float32), jnp.arange(GROUP_SIZE))
    return out_acc.astype(jnp.bfloat16)
```

```python
import functools

import jax
import jax.numpy as jnp
from jax import lax
from jax.experimental import pallas as pl
from jax.experimental.pallas import tpu as pltpu
from jax.sharding import PartitionSpec as P

MESH = pl.DeviceIdType.MESH
AXIS = "expert"
RIGHT, LEFT = 0, 1


def moe_kernel(
    n_chips,
    tok_hbm, ids_ref, wts_ref, dslot_ref, eslot_ref, wg_hbm, wu_hbm, wd_hbm,
    out_ref,
    xbuf, zbuf, zpart, leafbuf, sumbuf, recvbuf, meta, gate_col, hid, wg, wu, wd,
    load_sem, ag_send, ag_recv, mt_send, mt_recv, xd_send, xd_recv, md_send, md_recv,
    zd_send, zd_recv, lf_send, lf_recv, rs_send, rs_recv,
):
    me = lax.axis_index(AXIS)
    chip, core = me // 2, lax.rem(me, 2)
    mate = chip * 2 + 1 - core
    next_chip = (lax.rem(chip + 1, n_chips), lax.rem(chip + n_chips - 1, n_chips))
    far = n_chips // 2
    last = 2 * far - 1
    n_exp, d_model, d_ff = wg.shape
    half = xbuf.shape[1] // 4
    kind_rows = 2 * half
    sub = half // 2

    def rows(kind, way):
        return pl.ds(pl.multiple_of(kind * kind_rows + way * half, half), half)

    def krows(kind):
        return pl.ds(pl.multiple_of(kind * kind_rows, kind_rows), kind_rows)

    def remote(src, dst, send, recv, to):
        return pltpu.make_async_remote_copy(
            src_ref=src, dst_ref=dst, send_sem=send, recv_sem=recv, device_id={AXIS: to}, device_id_type=MESH
        )

    def ag_copy(step, way, src_i, src_way):
        return remote(
            xbuf.at[src_i, rows(core, src_way)], xbuf.at[step + 1, rows(core, way)],
            ag_send.at[step, way], ag_recv.at[step, way], next_chip[way] * 2 + core,
        )

    def mt_copy(hop, way):
        return remote(
            meta.at[hop, core, way], meta.at[hop + 1, core, way],
            mt_send.at[hop, way], mt_recv.at[hop, way], next_chip[way] * 2 + core,
        )

    def xd_copy(i, kind):
        return remote(xbuf.at[i, krows(kind)], xbuf.at[i, krows(kind)], xd_send.at[i], xd_recv.at[i], mate)

    def md_copy(hop, kind):
        return remote(meta.at[hop, kind], meta.at[hop, kind], md_send.at[hop], md_recv.at[hop], mate)

    def zd_copy(i):
        return remote(zbuf.at[i, krows(1 - core)], zpart.at[i], zd_send.at[i], zd_recv.at[i], mate)

    def leaf_copy(r, way, kind, src_core):
        i, side = (2 * far - 3, 1 - way) if r == 0 else (last, way)
        return remote(
            zbuf.at[i, rows(kind, side)], leafbuf.at[r, way, src_core],
            lf_send.at[r, way, kind], lf_recv.at[r, way, src_core], next_chip[way] * 2 + kind,
        )

    def rs_copy(r, way, s):
        part = pl.ds(s * sub, sub)
        return remote(
            sumbuf.at[r - 2, way, part], recvbuf.at[r - 2, way, part],
            rs_send.at[r - 2, way, s], rs_recv.at[r - 2, way, s], next_chip[way] * 2 + core,
        )

    loads = [
        pltpu.make_async_copy(tok_hbm, xbuf.at[0, krows(core)], load_sem.at[0]),
        pltpu.make_async_copy(wg_hbm, wg, load_sem.at[1]),
        pltpu.make_async_copy(wu_hbm, wu, load_sem.at[2]),
        pltpu.make_async_copy(wd_hbm, wd, load_sem.at[3]),
    ]
    loads[0].start()

    barrier = pltpu.get_barrier_semaphore()
    pl.semaphore_signal(barrier, inc=1, device_id={AXIS: mate}, device_id_type=MESH)
    for way in (RIGHT, LEFT):
        for kind in (0, 1):
            pl.semaphore_signal(barrier, inc=1, device_id={AXIS: next_chip[way] * 2 + kind}, device_id_type=MESH)
    for load in loads[1:]:
        load.start()

    kept = (dslot_ref[...] >= 0) & (eslot_ref[...] >= 0)
    expert = jnp.where(kept, ids_ref[...], -1).astype(jnp.float32)
    table = jnp.concatenate([wts_ref[...], expert], axis=0).astype(jnp.bfloat16)
    for way in (RIGHT, LEFT):
        meta[0, core, way] = table

    pl.semaphore_wait(barrier, 5)
    loads[0].wait()
    for way in (RIGHT, LEFT):
        ag_copy(0, way, 0, way).start()
        mt_copy(0, way).start()
    for way in (RIGHT, LEFT):
        ag_copy(1, way, 0, 1 - way).start()
    md_copy(0, core).start()
    xd_copy(0, core).start()
    for load in loads[1:]:
        load.wait()

    def arrive(i):
        odd = lax.rem(i, 2) == 1
        for way in (RIGHT, LEFT):
            ag_copy(i - 1, way, i, way).wait_recv()

            @pl.when(i <= last - 2)
            def _():
                ag_copy(i + 1, way, i, way).start()

        hop = (i + 1) // 2

        @pl.when(odd)
        def _():
            for way in (RIGHT, LEFT):
                mt_copy(hop - 1, way).wait_recv()

                @pl.when(hop < far)
                def _():
                    mt_copy(hop, way).start()

            md_copy(hop, core).start()

        xd_copy(i, core).start()

    def compute(i):
        hop = (i + 1) // 2
        fresh = (lax.rem(i, 2) == 1) | (i == 0)

        @pl.when(fresh)
        def _():
            md_copy(hop, 1 - core).wait_recv()
            lines = []
            for kind in (0, 1):
                for way in (RIGHT, LEFT):
                    both = meta[hop, kind, way].astype(jnp.float32)
                    top_k = both.shape[0] // 2
                    for e in range(n_exp):
                        mine = both[top_k:] == (me * n_exp + e).astype(jnp.float32)
                        lines.append(jnp.sum(jnp.where(mine, both[:top_k], 0.0), axis=0, keepdims=True))
            stacked = jnp.concatenate(lines, axis=0)
            gate_col[:, : len(lines)] = stacked.T

        xd_copy(i, 1 - core).wait_recv()
        x = xbuf[i]
        blk = 256
        for e in range(n_exp):
            for b in range(d_ff // blk):
                cols = pl.ds(b * blk, blk)
                g = jnp.dot(x, wg[e, :, cols], preferred_element_type=jnp.float32)
                u = jnp.dot(x, wu[e, :, cols], preferred_element_type=jnp.float32)
                hid[e, :, cols] = (jax.nn.silu(g) * u).astype(jnp.bfloat16)
        gates = []
        for e in range(n_exp):
            parts = []
            for kind in (0, 1):
                for way in (RIGHT, LEFT):
                    start = jnp.where(fresh, way, 1 - way) * half
                    col = (kind * 2 + way) * n_exp + e
                    parts.append(gate_col[pl.ds(pl.multiple_of(start, half), half), col : col + 1])
            gates.append(jnp.concatenate(parts, axis=0))
        for b in range(d_model // blk):
            cols = pl.ds(b * blk, blk)
            z = None
            for e in range(n_exp):
                y = jnp.dot(hid[e], wd[e, :, cols], preferred_element_type=jnp.float32)
                y = y.astype(jnp.bfloat16).astype(jnp.float32)
                term = jnp.where(gates[e] != 0.0, gates[e] * y, 0.0)
                z = term if z is None else z + term
            zbuf[i, :, cols] = z.astype(jnp.bfloat16)

    def send_leaf(r):
        for way in (RIGHT, LEFT):
            for kind in (0, 1):
                leaf_copy(r, way, kind, core).start()

    def step(i, carry):
        @pl.when(i <= last - 2)
        def _():
            arrive(i)

        @pl.when(i == last)
        def _():
            arrive(i - 1)
            arrive(i)

        done = i - 1
        compute(done)

        @pl.when(done == last - 2)
        def _():
            send_leaf(0)

        @pl.when(done == last)
        def _():
            send_leaf(1)

        @pl.when((done != last - 2) & (done != last))
        def _():
            zd_copy(done).start()

        return carry

    lax.fori_loop(1, last + 2, step, 0)

    block_of = []
    for r in range(last):
        if r == last - 1:
            block_of.append(2)
        elif r % 2 == 0:
            block_of.append(2 * (far - 1 - r // 2) - 1)
        else:
            block_of.append(last if r == 1 else 2 * (far - r // 2))

    for r in range(2, last):
        i = block_of[r]
        zd_copy(i).wait_recv()
        src = r - 1 if r == last - 1 else r - 2
        for s in range(2):
            for way in (RIGHT, LEFT):
                side = 1 - way
                part = pl.ds(s * sub, sub)
                if src < 2:
                    if s == 0:
                        for kind in (0, 1):
                            leaf_copy(src, way, core, kind).wait_recv()
                    acc = leafbuf[src, way, 0, part].astype(jnp.float32) + leafbuf[src, way, 1, part].astype(jnp.float32)
                else:
                    rs_copy(src, way, s).wait_recv()
                    acc = recvbuf[src - 2, way, part]
                own = pl.ds(pl.multiple_of(core * kind_rows + side * half + s * sub, sub), sub)
                acc = acc + zbuf[i, own, :].astype(jnp.float32)
                acc = acc + zpart[i, pl.ds(side * half + s * sub, sub), :].astype(jnp.float32)
                sumbuf[r - 2, way, part] = acc
                rs_copy(r, way, s).start()

    zd_copy(0).wait_recv()
    for s in range(2):
        for way in (RIGHT, LEFT):
            rs_copy(last - 3, way, s).wait_recv()
    for s in range(2):
        for h in (0, 1):
            part = pl.ds(s * sub, sub)
            rs_copy(last - 1, h, s).wait_recv()
            own = pl.ds(pl.multiple_of(core * kind_rows + h * half + s * sub, sub), sub)
            acc = recvbuf[last - 3, h, part] + recvbuf[last - 5, 1 - h, part]
            acc = acc + zbuf[0, own, :].astype(jnp.float32)
            acc = acc + zpart[0, pl.ds(h * half + s * sub, sub), :].astype(jnp.float32)
            out_ref[pl.ds(h * half + s * sub, sub), :] = acc.astype(out_ref.dtype)

    for way in (RIGHT, LEFT):
        for n in range(last):
            ag_copy(n, way, 0, way).wait_send()
        for hop in range(far):
            mt_copy(hop, way).wait_send()
        for r in (0, 1):
            for kind in (0, 1):
                leaf_copy(r, way, kind, core).wait_send()
        for r in range(2, last):
            for s in range(2):
                rs_copy(r, way, s).wait_send()
    for i in range(last + 1):
        xd_copy(i, core).wait_send()
        if i not in (last - 2, last):
            zd_copy(i).wait_send()
    for hop in range(far + 1):
        md_copy(hop, core).wait_send()


def solution(mesh):
    groups = mesh.shape[AXIS]
    n_chips = groups // 2
    far = n_chips // 2
    last = 2 * far - 1
    row_spec = P(("data", "expert"), None)
    weight_spec = P("expert", None, None)

    def device_layer(tokens, expert_ids, gate_wts, dev_slot, exp_slot, w_gate, w_up, w_down):
        tok_dev, top_k = expert_ids.shape
        d_model = tokens.shape[1]
        e_local, _, d_ff = w_gate.shape
        half = tok_dev // 2
        bf16, f32 = jnp.bfloat16, jnp.float32
        dma = pltpu.SemaphoreType.DMA
        vmem = pl.BlockSpec(memory_space=pltpu.VMEM)
        hbm = pl.BlockSpec(memory_space=pl.ANY)
        return pl.pallas_call(
            functools.partial(moe_kernel, n_chips),
            out_shape=jax.ShapeDtypeStruct((tok_dev, d_model), bf16),
            in_specs=[hbm] + [vmem] * 4 + [hbm] * 3,
            out_specs=vmem,
            scratch_shapes=[
                pltpu.VMEM((last + 1, 4 * half, d_model), bf16),
                pltpu.VMEM((last + 1, 4 * half, d_model), bf16),
                pltpu.VMEM((last + 1, 2 * half, d_model), bf16),
                pltpu.VMEM((2, 2, 2, half, d_model), bf16),
                pltpu.VMEM((last - 2, 2, half, d_model), f32),
                pltpu.VMEM((last - 2, 2, half, d_model), f32),
                pltpu.VMEM((far + 1, 2, 2, 2 * top_k, tok_dev), bf16),
                pltpu.VMEM((tok_dev, 128), f32),
                pltpu.VMEM((e_local, 4 * half, d_ff), bf16),
                pltpu.VMEM(w_gate.shape, bf16),
                pltpu.VMEM(w_up.shape, bf16),
                pltpu.VMEM(w_down.shape, bf16),
                dma((4,)),
                dma((last, 2)), dma((last, 2)),
                dma((far, 2)), dma((far, 2)),
                dma((last + 1,)), dma((last + 1,)),
                dma((far + 1,)), dma((far + 1,)),
                dma((last + 1,)), dma((last + 1,)),
                dma((2, 2, 2)), dma((2, 2, 2)),
                dma((last - 2, 2, 2)), dma((last - 2, 2, 2)),
            ],
            compiler_params=pltpu.CompilerParams(
                collective_id=0, has_side_effects=True, vmem_limit_bytes=56 * 1024 * 1024
            ),
        )(tokens, expert_ids.T, gate_wts.T, dev_slot.T, exp_slot.T, w_gate, w_up, w_down)

    def moe_layer(tokens, expert_ids, gate_wts, dev_slot, exp_slot, w_gate, w_up, w_down):
        mapped = jax.shard_map(device_layer, mesh=mesh, in_specs=(row_spec,) * 5 + (weight_spec,) * 3, out_specs=row_spec, check_vma=False)
        return mapped(tokens, expert_ids, gate_wts, dev_slot, exp_slot, w_gate, w_up, w_down)

    return moe_layer
```

```python
import functools

import jax
import jax.numpy as jnp
from jax import lax
from jax.experimental import pallas as pl
from jax.experimental.pallas import tpu as pltpu
from jax.sharding import PartitionSpec as P

MESH = pl.DeviceIdType.MESH
AXIS = "expert"
RIGHT, LEFT = 0, 1


def moe_kernel(
    n_chips,
    tok_hbm, ids_hbm, wts_hbm, dslot_hbm, eslot_hbm, wg_hbm, wu_hbm, wd_hbm,
    out_ref,
    xbuf, zbuf, zpart, packbuf, leafbuf, sumbuf, recvbuf, meta, gate_col, hid, wg, wu, wd, ids, wts, dslot, eslot,
    load_sem, ag_send, ag_recv, mt_send, mt_recv, xd_send, xd_recv, md_send, md_recv,
    zd_send, zd_recv, lf_send, lf_recv, rs_send, rs_recv,
):
    me = lax.axis_index(AXIS)
    chip, core = me // 2, lax.rem(me, 2)
    mate = chip * 2 + 1 - core
    next_chip = (lax.rem(chip + 1, n_chips), lax.rem(chip + n_chips - 1, n_chips))
    far = n_chips // 2
    last = 2 * far - 1
    n_exp, d_model, d_ff = wg.shape
    n_tok = xbuf.shape[1] // 2
    half = n_tok // 2
    cap = leafbuf.shape[-2]
    wide = d_model // 2
    top_k = ids.shape[0]
    bf16, f32 = jnp.bfloat16, jnp.float32

    def rows(kind, side):
        return pl.ds(pl.multiple_of(kind * n_tok + side * half, half), half)

    def krows(kind):
        return pl.ds(pl.multiple_of(kind * n_tok, n_tok), n_tok)

    def remote(src, dst, send, recv, to):
        return pltpu.make_async_remote_copy(
            src_ref=src, dst_ref=dst, send_sem=send, recv_sem=recv, device_id={AXIS: to}, device_id_type=MESH
        )

    def ag_copy(step, way, src_i, src_side):
        return remote(
            xbuf.at[src_i, rows(core, src_side)], xbuf.at[step + 1, rows(core, way)],
            ag_send.at[step, way], ag_recv.at[step, way], next_chip[way] * 2 + core,
        )

    def mt_copy(hop, way):
        return remote(
            meta.at[hop, core, way], meta.at[hop + 1, core, way],
            mt_send.at[hop, way], mt_recv.at[hop, way], next_chip[way] * 2 + core,
        )

    def xd_copy(i, kind):
        return remote(xbuf.at[i, krows(kind)], xbuf.at[i, krows(kind)], xd_send.at[i], xd_recv.at[i], mate)

    def md_copy(hop, kind):
        return remote(meta.at[hop, kind], meta.at[hop, kind], md_send.at[hop], md_recv.at[hop], mate)

    def zd_copy(i):
        return remote(zbuf.at[i, krows(1 - core)], zpart.at[i], zd_send.at[i], zd_recv.at[i], mate)

    def leaf_copy(r, way, kind, src_core):
        return remote(
            packbuf.at[r, way, kind], leafbuf.at[r, way, src_core],
            lf_send.at[r, way, kind], lf_recv.at[r, way, src_core], next_chip[way] * 2 + kind,
        )

    def n_sub(r):
        return 1 if r < last - 2 else 2

    def rs_copy(r, way, s):
        n = n_tok // n_sub(r)
        part = pl.ds(s * n, n)
        return remote(
            sumbuf.at[r - 2, way, part], recvbuf.at[r - 2, way, part],
            rs_send.at[r - 2, way, s], rs_recv.at[r - 2, way, s], next_chip[way] * 2 + core,
        )

    loads = [
        pltpu.make_async_copy(a, b, load_sem.at[j])
        for j, (a, b) in enumerate(
            (
                (tok_hbm, xbuf.at[0, krows(core)]), (ids_hbm, ids), (wts_hbm, wts), (dslot_hbm, dslot), (eslot_hbm, eslot),
                (wg_hbm, wg), (wu_hbm, wu), (wd_hbm, wd),
            )
        )
    ]
    loads[0].start()
    barrier = pltpu.get_barrier_semaphore()
    pl.semaphore_signal(barrier, inc=1, device_id={AXIS: mate}, device_id_type=MESH)
    for way in (RIGHT, LEFT):
        for kind in (0, 1):
            pl.semaphore_signal(barrier, inc=1, device_id={AXIS: next_chip[way] * 2 + kind}, device_id_type=MESH)
    for load in loads[1:]:
        load.start()
    loads[0].wait()
    pl.semaphore_wait(barrier, 5)

    for way in (RIGHT, LEFT):
        ag_copy(0, way, 0, way).start()
    for load in loads[1:5]:
        load.wait()
    kept = (dslot[...] >= 0) & (eslot[...] >= 0)
    expert = jnp.where(kept, ids[...], -1).astype(f32)
    table = jnp.concatenate([wts[...], expert], axis=0).astype(bf16)
    for way in (RIGHT, LEFT):
        meta[0, core, way] = table
    for way in (RIGHT, LEFT):
        mt_copy(0, way).start()
    for way in (RIGHT, LEFT):
        ag_copy(1, way, 0, 1 - way).start()
    for load in loads[5:]:
        load.wait()

    def experts_of(hop, kind, side):
        return meta[hop, kind, side].astype(f32)[top_k:]

    def routed(expert, device):
        hits = sum(
            jnp.sum((expert == (device * n_exp + e).astype(f32)).astype(f32), axis=0, keepdims=True) for e in range(n_exp)
        )
        return hits > 0.0

    def ranks(masks):
        lines = [m.astype(f32) for m in masks] + [jnp.zeros((8 - len(masks), n_tok), f32)]
        before = lax.broadcasted_iota(jnp.int32, (n_tok, n_tok), 0) < lax.broadcasted_iota(jnp.int32, (n_tok, n_tok), 1)
        return jnp.dot(jnp.concatenate(lines, axis=0).astype(bf16), before.astype(bf16), preferred_element_type=f32)

    def packer(mask, rank):
        place = lax.broadcasted_iota(jnp.int32, (cap, n_tok), 0).astype(f32)
        return jnp.where(mask & (place == rank), 1.0, 0.0)

    def halves(j, side):
        return (2 * j - 1, 2 * j) if side == RIGHT else (2 * j, 2 * j - 1)

    def arrive(i):
        for way in (RIGHT, LEFT):
            ag_copy(i - 1, way, i, way).wait_recv()

            @pl.when(i <= last - 2)
            def _():
                ag_copy(i + 1, way, i, way).start()

        @pl.when(lax.rem(i, 2) == 1)
        def _():
            hop = (i + 1) // 2
            for way in (RIGHT, LEFT):
                mt_copy(hop - 1, way).wait_recv()

                @pl.when(hop < far)
                def _():
                    mt_copy(hop, way).start()

    def compute(i, kind, fresh):
        hop = (i + 1) // 2

        @pl.when(fresh)
        def _():
            lines = []
            for side in (RIGHT, LEFT):
                both = meta[hop, kind, side].astype(f32)
                for e in range(n_exp):
                    mine = both[top_k:] == (me * n_exp + e).astype(f32)
                    lines.append(jnp.sum(jnp.where(mine, both[:top_k], 0.0), axis=0, keepdims=True))
            lines.append(jnp.zeros((8 - len(lines), n_tok), f32))
            gate_col[kind, :, :8] = jnp.concatenate(lines, axis=0).T

        x = xbuf[i, krows(kind)]
        blk = 256
        for e in range(n_exp):
            for b in range(d_ff // blk):
                cols = pl.ds(b * blk, blk)
                g = jnp.dot(x, wg[e, :, cols], preferred_element_type=f32)
                u = jnp.dot(x, wu[e, :, cols], preferred_element_type=f32)
                hid[e, :, cols] = (jax.nn.silu(g) * u).astype(bf16)
        gates = []
        for e in range(n_exp):
            parts = []
            for side in (RIGHT, LEFT):
                start = jnp.where(fresh, side, 1 - side) * half
                col = side * n_exp + e
                parts.append(gate_col[kind, pl.ds(pl.multiple_of(start, half), half), col : col + 1])
            gates.append(jnp.concatenate(parts, axis=0))
        for b in range(d_model // blk):
            cols = pl.ds(b * blk, blk)
            z = None
            for e in range(n_exp):
                y = jnp.dot(hid[e], wd[e, :, cols], preferred_element_type=f32)
                y = y.astype(bf16).astype(f32)
                term = jnp.where(gates[e] != 0.0, gates[e] * y, 0.0)
                z = term if z is None else z + term
            zbuf[i, krows(kind), cols] = z.astype(bf16)

    def send_leaf(r, kind):
        if r == 0:
            masks = [routed(experts_of(far - 1, kind, 1 - way), me) for way in (RIGHT, LEFT)]
        else:
            masks = [routed(experts_of(far, kind, RIGHT), me)]
        rank = ranks(masks)
        for way in (RIGHT, LEFT):
            if r == 0:
                n, side, h = way, 1 - way, 1 - way
                places = [(i, side) for i in halves(far - 1, side)]
            else:
                n, h = 0, way
                places = [(last, RIGHT), (last, LEFT)]
            pick = packer(masks[n], rank[n : n + 1]).astype(bf16)
            cols = pl.ds(h * wide, wide)
            z = jnp.concatenate([zbuf[i, rows(kind, side), cols] for i, side in places], axis=0)
            packbuf[r, way, kind] = jnp.dot(pick, z, preferred_element_type=f32).astype(bf16)
            leaf_copy(r, way, kind, core).start()

    def step(i, carry):
        odd = lax.rem(i, 2) == 1
        fresh = odd | (i == 0)

        @pl.when(i >= 1)
        def _():
            arrive(i)

        xd_copy(i, core).start()

        @pl.when(fresh)
        def _():
            md_copy((i + 1) // 2, core).start()

        def one_kind(turn, carry):
            kind = lax.rem(core + turn, 2)

            @pl.when(turn == 1)
            def _():
                xd_copy(i, 1 - core).wait_recv()

                @pl.when(fresh)
                def _():
                    md_copy((i + 1) // 2, 1 - core).wait_recv()

            compute(i, kind, fresh)

            @pl.when(i == last - 1)
            def _():
                send_leaf(0, kind)

            @pl.when(i == last)
            def _():
                send_leaf(1, kind)

            return carry

        lax.fori_loop(0, 2, one_kind, 0)

        @pl.when(i < last)
        def _():
            zd_copy(i).start()

        return carry

    lax.fori_loop(0, last + 1, step, 0)

    def plan(r, way):
        if r == last - 1:
            return 1, way
        return (far - 1 - r // 2, 1 - way) if r % 2 == 0 else (far - r // 2, way)

    def unpack(r, way):
        j, _ = plan(r, way)
        expert = experts_of(j - 1, core, 1 - way)
        masks = [routed(expert, next_chip[1 - way] * 2 + k) for k in (0, 1)]
        rank = ranks(masks)
        picks = [packer(masks[k], rank[k : k + 1]).T.astype(bf16) for k in (0, 1)]
        for k in (0, 1):
            leaf_copy(r, way, core, k).wait_recv()
        return sum(jnp.dot(picks[k], leafbuf[r, way, k], preferred_element_type=f32) for k in (0, 1))

    known = set()
    for r in range(2, last):
        src = r - 1 if r == last - 1 else r - 2
        for i in halves(plan(r, RIGHT)[0], RIGHT):
            if i not in known:
                known.add(i)
                zd_copy(i).wait_recv()
        for t in (0, 1):
            for way in (RIGHT, LEFT):
                j, h = plan(r, way)
                side = 1 - way
                i = halves(j, side)[t]
                part, cols = pl.ds(t * half, half), pl.ds(h * wide, wide)
                if src < 2:
                    if t == 0:
                        sumbuf[r - 2, way] = unpack(src, way)
                    acc = sumbuf[r - 2, way, part]
                else:
                    if t < n_sub(src):
                        rs_copy(src, way, t).wait_recv()
                    acc = recvbuf[src - 2, way, part]
                acc = acc + zbuf[i, rows(core, side), cols].astype(f32)
                acc = acc + zpart[i, pl.ds(side * half, half), cols].astype(f32)
                sumbuf[r - 2, way, part] = acc
                if n_sub(r) == 2:
                    rs_copy(r, way, t).start()
                elif t == 1:
                    rs_copy(r, way, 0).start()

    zd_copy(0).wait_recv()
    for way in (RIGHT, LEFT):
        rs_copy(last - 3, way, 0).wait_recv()
    for t in (0, 1):
        for way in (RIGHT, LEFT):
            part, cols = pl.ds(t * half, half), pl.ds(way * wide, wide)
            rs_copy(last - 1, way, t).wait_recv()
            acc = recvbuf[last - 3, way, part] + recvbuf[last - 5, 1 - way, part]
            acc = acc + zbuf[0, rows(core, t), cols].astype(f32)
            acc = acc + zpart[0, part, cols].astype(f32)
            out_ref[part, cols] = acc.astype(out_ref.dtype)

    for way in (RIGHT, LEFT):
        for n in range(last):
            ag_copy(n, way, 0, way).wait_send()
        for hop in range(far):
            mt_copy(hop, way).wait_send()
        for r in (0, 1):
            for kind in (0, 1):
                leaf_copy(r, way, kind, core).wait_send()
        for r in range(2, last):
            for s in range(n_sub(r)):
                rs_copy(r, way, s).wait_send()
    for i in range(last + 1):
        xd_copy(i, core).wait_send()
        if i < last:
            zd_copy(i).wait_send()
    for hop in range(far + 1):
        md_copy(hop, core).wait_send()


def solution(mesh):
    groups = mesh.shape[AXIS]
    n_chips = groups // 2
    far = n_chips // 2
    last = 2 * far - 1
    row_spec = P(("data", "expert"), None)
    weight_spec = P("expert", None, None)

    def device_layer(tokens, expert_ids, gate_wts, dev_slot, exp_slot, w_gate, w_up, w_down):
        tok_dev, top_k = expert_ids.shape
        d_model = tokens.shape[1]
        e_local, _, d_ff = w_gate.shape
        dev_cap = min(tok_dev, 8 * ((3 * tok_dev * top_k + 16 * groups - 1) // (16 * groups)))
        bf16, f32, i32 = jnp.bfloat16, jnp.float32, jnp.int32
        dma = pltpu.SemaphoreType.DMA
        args = (tokens, expert_ids.T, gate_wts.T, dev_slot.T, exp_slot.T, w_gate, w_up, w_down)
        args = [pltpu.with_memory_space_constraint(a, pltpu.HBM) for a in args]
        return pl.pallas_call(
            functools.partial(moe_kernel, n_chips),
            out_shape=jax.ShapeDtypeStruct((tok_dev, d_model), bf16),
            in_specs=[pl.BlockSpec(memory_space=pltpu.HBM)] * len(args),
            out_specs=pl.BlockSpec(memory_space=pltpu.VMEM),
            scratch_shapes=[
                pltpu.VMEM((last + 1, 2 * tok_dev, d_model), bf16),
                pltpu.VMEM((last + 1, 2 * tok_dev, d_model), bf16),
                pltpu.VMEM((last, tok_dev, d_model), bf16),
                pltpu.VMEM((2, 2, 2, dev_cap, d_model // 2), bf16),
                pltpu.VMEM((2, 2, 2, dev_cap, d_model // 2), bf16),
                pltpu.VMEM((last - 2, 2, tok_dev, d_model // 2), f32),
                pltpu.VMEM((last - 2, 2, tok_dev, d_model // 2), f32),
                pltpu.VMEM((far + 1, 2, 2, 2 * top_k, tok_dev), bf16),
                pltpu.VMEM((2, tok_dev, 128), f32),
                pltpu.VMEM((e_local, tok_dev, d_ff), bf16),
                pltpu.VMEM(w_gate.shape, bf16),
                pltpu.VMEM(w_up.shape, bf16),
                pltpu.VMEM(w_down.shape, bf16),
                pltpu.VMEM((top_k, tok_dev), i32),
                pltpu.VMEM((top_k, tok_dev), f32),
                pltpu.VMEM((top_k, tok_dev), i32),
                pltpu.VMEM((top_k, tok_dev), i32),
                dma((8,)),
                dma((last, 2)), dma((last, 2)),
                dma((far, 2)), dma((far, 2)),
                dma((last + 1,)), dma((last + 1,)),
                dma((far + 1,)), dma((far + 1,)),
                dma((last,)), dma((last,)),
                dma((2, 2, 2)), dma((2, 2, 2)),
                dma((last - 2, 2, 2)), dma((last - 2, 2, 2)),
            ],
            compiler_params=pltpu.CompilerParams(
                collective_id=0, has_side_effects=True, vmem_limit_bytes=48 * 1024 * 1024
            ),
        )(*args)

    def moe_layer(tokens, expert_ids, gate_wts, dev_slot, exp_slot, w_gate, w_up, w_down):
        mapped = jax.shard_map(device_layer, mesh=mesh, in_specs=(row_spec,) * 5 + (weight_spec,) * 3, out_specs=row_spec, check_vma=False)
        return mapped(tokens, expert_ids, gate_wts, dev_slot, exp_slot, w_gate, w_up, w_down)

    return moe_layer
```

```python
import functools

import jax
import jax.numpy as jnp
from jax import lax
from jax.experimental import pallas as pl
from jax.experimental.pallas import tpu as pltpu
from jax.sharding import PartitionSpec as P

MESH = pl.DeviceIdType.MESH
AXIS = "expert"
RIGHT, LEFT = 0, 1


def moe_kernel(
    n_chips,
    tok_hbm, ids_hbm, wts_hbm, dslot_hbm, eslot_hbm, wg_hbm, wu_hbm, wd_hbm,
    out_ref,
    xbuf, zbuf, zpart, packbuf, leafbuf, sumbuf, recvbuf, meta, gate_col, picks, hid, w_in, wd, ids, wts, dslot, eslot,
    load_sem, ag_send, ag_recv, mt_send, mt_recv, xd_send, xd_recv, md_send, md_recv,
    zd_send, zd_recv, lf_send, lf_recv, rs_send, rs_recv,
):
    me = lax.axis_index(AXIS)
    chip, core = me // 2, lax.rem(me, 2)
    mate = chip * 2 + 1 - core
    next_chip = (lax.rem(chip + 1, n_chips), lax.rem(chip + n_chips - 1, n_chips))
    far = n_chips // 2
    last = 2 * far - 1
    _, n_exp, d_model, d_ff = w_in.shape
    n_tok = xbuf.shape[1] // 2
    half = n_tok // 2
    cap = leafbuf.shape[-2]
    wide = d_model // 2
    top_k = ids.shape[0]
    bf16, f32 = jnp.bfloat16, jnp.float32

    def rows(kind, side):
        return pl.ds(pl.multiple_of(kind * n_tok + side * half, half), half)

    def krows(kind):
        return pl.ds(pl.multiple_of(kind * n_tok, n_tok), n_tok)

    def remote(src, dst, send, recv, to):
        return pltpu.make_async_remote_copy(
            src_ref=src, dst_ref=dst, send_sem=send, recv_sem=recv, device_id={AXIS: to}, device_id_type=MESH
        )

    def ag_copy(step, way, src_i, src_side):
        return remote(
            xbuf.at[src_i, rows(core, src_side)], xbuf.at[step + 1, rows(core, way)],
            ag_send, ag_recv.at[step, way], next_chip[way] * 2 + core,
        )

    def mt_copy(hop, way):
        return remote(
            meta.at[hop, core, way], meta.at[hop + 1, core, way],
            mt_send, mt_recv.at[hop], next_chip[way] * 2 + core,
        )

    def xd_copy(i, kind):
        return remote(xbuf.at[i, krows(kind)], xbuf.at[i, krows(kind)], xd_send, xd_recv.at[i], mate)

    def md_copy(hop, kind):
        return remote(meta.at[hop, kind], meta.at[hop, kind], md_send, md_recv.at[hop], mate)

    def zd_copy(i):
        return remote(zbuf.at[i, krows(1 - core)], zpart.at[i], zd_send, zd_recv, mate)

    def leaf_copy(r, way, kind, src_core):
        return remote(
            packbuf.at[r, way, kind], leafbuf.at[r, way, src_core],
            lf_send, lf_recv.at[r, way], next_chip[way] * 2 + kind,
        )

    def n_sub(r):
        return 1 if r < last - 2 else 2

    def rs_slot(r, way, s):
        if n_sub(r) == 1:
            return r - 2
        return last - 4 + (r - last + 2) * 4 + s * 2 + way

    def rs_copy(r, way, s):
        n = n_tok // n_sub(r)
        part = pl.ds(s * n, n)
        return remote(
            sumbuf.at[r - 2, way, part], recvbuf.at[r - 2, way, part],
            rs_send, rs_recv.at[rs_slot(r, way, s)], next_chip[way] * 2 + core,
        )

    def drain(ref, sem):
        pltpu.make_async_copy(ref, ref, sem).wait()

    loads = [
        pltpu.make_async_copy(a, b, load_sem.at[j])
        for a, b, j in (
            (tok_hbm, xbuf.at[0, krows(core)], 0),
            (ids_hbm, ids, 1), (wts_hbm, wts, 1), (dslot_hbm, dslot, 1), (eslot_hbm, eslot, 1),
            (wg_hbm, w_in.at[0], 2), (wu_hbm, w_in.at[1], 2), (wd_hbm, wd, 3),
        )
    ]
    loads[0].start()
    barrier = pltpu.get_barrier_semaphore()
    pl.semaphore_signal(barrier, inc=1, device_id={AXIS: mate}, device_id_type=MESH)
    for way in (RIGHT, LEFT):
        for kind in (0, 1):
            pl.semaphore_signal(barrier, inc=1, device_id={AXIS: next_chip[way] * 2 + kind}, device_id_type=MESH)
    for load in loads[1:]:
        load.start()
    loads[0].wait()
    pl.semaphore_wait(barrier, 5)

    for way in (RIGHT, LEFT):
        ag_copy(0, way, 0, way).start()
    drain(gate_col.at[0, : 4 * top_k], load_sem.at[1])
    kept = (dslot[...] >= 0) & (eslot[...] >= 0)
    expert = jnp.where(kept, ids[...], -1).astype(f32)
    table = jnp.concatenate([wts[...], expert], axis=0).astype(bf16)
    for way in (RIGHT, LEFT):
        meta[0, core, way] = table
    for way in (RIGHT, LEFT):
        mt_copy(0, way).start()
    for way in (RIGHT, LEFT):
        ag_copy(1, way, 0, 1 - way).start()
    drain(w_in, load_sem.at[2])
    loads[7].wait()

    def experts_of(hop, kind, side):
        return meta[hop, kind, side].astype(f32)[top_k:]

    def routed(expert, device):
        hits = sum(
            jnp.sum((expert == (device * n_exp + e).astype(f32)).astype(f32), axis=0, keepdims=True) for e in range(n_exp)
        )
        return hits > 0.0

    def ranks(masks):
        lines = [m.astype(f32) for m in masks] + [jnp.zeros((8 - len(masks), n_tok), f32)]
        before = lax.broadcasted_iota(jnp.int32, (n_tok, n_tok), 0) < lax.broadcasted_iota(jnp.int32, (n_tok, n_tok), 1)
        return jnp.dot(jnp.concatenate(lines, axis=0).astype(bf16), before.astype(bf16), preferred_element_type=f32)

    def packer(mask, rank):
        place = lax.broadcasted_iota(jnp.int32, (cap, n_tok), 0).astype(f32)
        return jnp.where(mask & (place == rank), 1.0, 0.0)

    def halves(j, side):
        return (2 * j - 1, 2 * j) if side == RIGHT else (2 * j, 2 * j - 1)

    def arrive(i):
        for way in (RIGHT, LEFT):
            ag_copy(i - 1, way, i, way).wait_recv()

            @pl.when(i <= last - 2)
            def _():
                ag_copy(i + 1, way, i, way).start()

        @pl.when(lax.rem(i, 2) == 1)
        def _():
            hop = (i + 1) // 2
            drain(meta.at[hop, core], mt_recv.at[hop - 1])

            @pl.when(hop < far)
            def _():
                for way in (RIGHT, LEFT):
                    mt_copy(hop, way).start()

    def compute(i, kind, fresh):
        hop = (i + 1) // 2

        @pl.when(fresh)
        def _():
            lines = []
            for side in (RIGHT, LEFT):
                both = meta[hop, kind, side].astype(f32)
                for e in range(n_exp):
                    mine = both[top_k:] == (me * n_exp + e).astype(f32)
                    lines.append(jnp.sum(jnp.where(mine, both[:top_k], 0.0), axis=0, keepdims=True))
            lines.append(jnp.zeros((8 - len(lines), n_tok), f32))
            gate_col[kind, :, :8] = jnp.concatenate(lines, axis=0).T

        x = xbuf[i, krows(kind)]
        blk = 256
        for e in range(n_exp):
            for b in range(d_ff // blk):
                cols = pl.ds(b * blk, blk)
                g = jnp.dot(x, w_in[0, e, :, cols], preferred_element_type=f32)
                u = jnp.dot(x, w_in[1, e, :, cols], preferred_element_type=f32)
                hid[e, :, cols] = (jax.nn.silu(g) * u).astype(bf16)
        gates = []
        for e in range(n_exp):
            parts = []
            for side in (RIGHT, LEFT):
                start = jnp.where(fresh, side, 1 - side) * half
                col = side * n_exp + e
                parts.append(gate_col[kind, pl.ds(pl.multiple_of(start, half), half), col : col + 1])
            gates.append(jnp.concatenate(parts, axis=0))
        for b in range(d_model // blk):
            cols = pl.ds(b * blk, blk)
            z = None
            for e in range(n_exp):
                y = jnp.dot(hid[e], wd[e, :, cols], preferred_element_type=f32)
                y = y.astype(bf16).astype(f32)
                term = jnp.where(gates[e] != 0.0, gates[e] * y, 0.0)
                z = term if z is None else z + term
            zbuf[i, krows(kind), cols] = z.astype(bf16)

    def prepare(r, kind):
        if r == 0:
            masks = [routed(experts_of(far - 1, kind, 1 - way), me) for way in (RIGHT, LEFT)]
        else:
            masks = [routed(experts_of(far, kind, RIGHT), me)] * 2
        rank = ranks(masks)
        for way in (RIGHT, LEFT):
            picks[kind, way] = packer(masks[way], rank[way : way + 1]).astype(bf16)

    def send_leaf(r, kind):
        for way in (RIGHT, LEFT):
            if r == 0:
                side, h = 1 - way, 1 - way
                places = [(i, side) for i in halves(far - 1, side)]
            else:
                h = way
                places = [(last, RIGHT), (last, LEFT)]
            cols = pl.ds(h * wide, wide)
            z = jnp.concatenate([zbuf[i, rows(kind, side), cols] for i, side in places], axis=0)
            packbuf[r, way, kind] = jnp.dot(picks[kind, way], z, preferred_element_type=f32).astype(bf16)
            leaf_copy(r, way, kind, core).start()

    def step(i, carry):
        odd = lax.rem(i, 2) == 1
        fresh = odd | (i == 0)

        @pl.when(i >= 1)
        def _():
            arrive(i)

        xd_copy(i, core).start()

        @pl.when(fresh)
        def _():
            md_copy((i + 1) // 2, core).start()

        def one_kind(turn, carry):
            kind = lax.rem(core + turn, 2)

            @pl.when(turn == 1)
            def _():
                xd_copy(i, 1 - core).wait_recv()

                @pl.when(fresh)
                def _():
                    md_copy((i + 1) // 2, 1 - core).wait_recv()

            @pl.when(i == last)
            def _():
                prepare(1, kind)

            compute(i, kind, fresh)

            @pl.when(i == last - 2)
            def _():
                prepare(0, kind)

            @pl.when(i == last - 1)
            def _():
                send_leaf(0, kind)

            @pl.when(i == last)
            def _():
                send_leaf(1, kind)

            return carry

        lax.fori_loop(0, 2, one_kind, 0)

        @pl.when(i < last)
        def _():
            zd_copy(i).start()

        return carry

    lax.fori_loop(0, last + 1, step, 0)

    def plan(r, way):
        if r == last - 1:
            return 1, way
        return (far - 1 - r // 2, 1 - way) if r % 2 == 0 else (far - r // 2, way)

    def unpack(r, way):
        j, _ = plan(r, way)
        expert = experts_of(j - 1, core, 1 - way)
        masks = [routed(expert, next_chip[1 - way] * 2 + k) for k in (0, 1)]
        rank = ranks(masks)
        picks = [packer(masks[k], rank[k : k + 1]).T.astype(bf16) for k in (0, 1)]
        drain(leafbuf.at[r, way], lf_recv.at[r, way])
        return sum(jnp.dot(picks[k], leafbuf[r, way, k], preferred_element_type=f32) for k in (0, 1))

    drain(zpart, zd_recv)
    for r in range(2, last):
        src = r - 1 if r == last - 1 else r - 2
        if 2 <= src < last - 2:
            drain(recvbuf.at[src - 2], rs_recv.at[src - 2])
        for t in (0, 1):
            for way in (RIGHT, LEFT):
                j, h = plan(r, way)
                side = 1 - way
                i = halves(j, side)[t]
                part, cols = pl.ds(t * half, half), pl.ds(h * wide, wide)
                if src < 2:
                    if t == 0:
                        sumbuf[r - 2, way] = unpack(src, way)
                    acc = sumbuf[r - 2, way, part]
                else:
                    if n_sub(src) == 2:
                        rs_copy(src, way, t).wait_recv()
                    acc = recvbuf[src - 2, way, part]
                acc = acc + zbuf[i, rows(core, side), cols].astype(f32)
                acc = acc + zpart[i, pl.ds(side * half, half), cols].astype(f32)
                sumbuf[r - 2, way, part] = acc
                if n_sub(r) == 2:
                    rs_copy(r, way, t).start()
                elif t == 1:
                    rs_copy(r, way, 0).start()

    drain(recvbuf.at[last - 5], rs_recv.at[last - 5])
    for t in (0, 1):
        for way in (RIGHT, LEFT):
            part, cols = pl.ds(t * half, half), pl.ds(way * wide, wide)
            rs_copy(last - 1, way, t).wait_recv()
            acc = recvbuf[last - 3, way, part] + recvbuf[last - 5, 1 - way, part]
            acc = acc + zbuf[0, rows(core, t), cols].astype(f32)
            acc = acc + zpart[0, part, cols].astype(f32)
            out_ref[part, cols] = acc.astype(out_ref.dtype)

    drain(xbuf.at[1:, :n_tok], ag_send)
    drain(meta.at[:far, 0], mt_send)
    drain(xbuf.at[:, :n_tok], xd_send)
    drain(meta.at[:, 0], md_send)
    drain(zpart, zd_send)
    drain(packbuf, lf_send)
    drain(sumbuf, rs_send)


def solution(mesh):
    groups = mesh.shape[AXIS]
    n_chips = groups // 2
    far = n_chips // 2
    last = 2 * far - 1
    row_spec = P(("data", "expert"), None)
    weight_spec = P("expert", None, None)

    def device_layer(tokens, expert_ids, gate_wts, dev_slot, exp_slot, w_gate, w_up, w_down):
        tok_dev, top_k = expert_ids.shape
        d_model = tokens.shape[1]
        e_local, _, d_ff = w_gate.shape
        dev_cap = min(tok_dev, 8 * ((3 * tok_dev * top_k + 16 * groups - 1) // (16 * groups)))
        bf16, f32, i32 = jnp.bfloat16, jnp.float32, jnp.int32
        dma = pltpu.SemaphoreType.DMA
        args = (tokens, expert_ids.T, gate_wts.T, dev_slot.T, exp_slot.T, w_gate, w_up, w_down)
        args = [pltpu.with_memory_space_constraint(a, pltpu.HBM) for a in args]
        return pl.pallas_call(
            functools.partial(moe_kernel, n_chips),
            out_shape=jax.ShapeDtypeStruct((tok_dev, d_model), bf16),
            in_specs=[pl.BlockSpec(memory_space=pltpu.HBM)] * len(args),
            out_specs=pl.BlockSpec(memory_space=pltpu.VMEM),
            scratch_shapes=[
                pltpu.VMEM((last + 1, 2 * tok_dev, d_model), bf16),
                pltpu.VMEM((last + 1, 2 * tok_dev, d_model), bf16),
                pltpu.VMEM((last, tok_dev, d_model), bf16),
                pltpu.VMEM((2, 2, 2, dev_cap, d_model // 2), bf16),
                pltpu.VMEM((2, 2, 2, dev_cap, d_model // 2), bf16),
                pltpu.VMEM((last - 2, 2, tok_dev, d_model // 2), f32),
                pltpu.VMEM((last - 2, 2, tok_dev, d_model // 2), f32),
                pltpu.VMEM((far + 1, 2, 2, 2 * top_k, tok_dev), bf16),
                pltpu.VMEM((2, tok_dev, 128), f32),
                pltpu.VMEM((2, 2, dev_cap, tok_dev), bf16),
                pltpu.VMEM((e_local, tok_dev, d_ff), bf16),
                pltpu.VMEM((2, *w_gate.shape), bf16),
                pltpu.VMEM(w_down.shape, bf16),
                pltpu.VMEM((top_k, tok_dev), i32),
                pltpu.VMEM((top_k, tok_dev), f32),
                pltpu.VMEM((top_k, tok_dev), i32),
                pltpu.VMEM((top_k, tok_dev), i32),
                dma((4,)),
                dma, dma((last, 2)),
                dma, dma((far,)),
                dma, dma((last + 1,)),
                dma, dma((far + 1,)),
                dma, dma,
                dma, dma((2, 2)),
                dma, dma((last + 4,)),
            ],
            compiler_params=pltpu.CompilerParams(
                collective_id=0, has_side_effects=True, vmem_limit_bytes=48 * 1024 * 1024
            ),
        )(*args)

    def moe_layer(tokens, expert_ids, gate_wts, dev_slot, exp_slot, w_gate, w_up, w_down):
        mapped = jax.shard_map(device_layer, mesh=mesh, in_specs=(row_spec,) * 5 + (weight_spec,) * 3, out_specs=row_spec, check_vma=False)
        return mapped(tokens, expert_ids, gate_wts, dev_slot, exp_slot, w_gate, w_up, w_down)

    return moe_layer
```

```python
import functools

import jax
import jax.numpy as jnp
from jax import lax
from jax.experimental import pallas as pl
from jax.experimental.pallas import tpu as pltpu
from jax.sharding import PartitionSpec as P

MESH = pl.DeviceIdType.MESH
AXIS = "expert"
RIGHT, LEFT = 0, 1


def chain_order(far):
    a, b, c, d = far + 1, far - 1, far, far - 2
    assert d == 2
    return [
(d, 2), (b, 3), (a, 5), (c, 4), (b, 2), (a, 4), (c, 3), (b, 1), (a, 3), (c, 2), (a, 2), (d, 1), (c, 1), (a, 1),
    ]


def moe_kernel(
    n_chips,
    tok_hbm, ids_hbm, wts_hbm, dslot_hbm, eslot_hbm, wg_hbm, wu_hbm, wd_hbm,
    out_ref,
    xbuf, zbuf, zpart, packbuf, leafbuf, sumbuf, recvbuf, meta, gate_col, picks, hid, w_in, wd, ids, wts, dslot, eslot,
    load_sem, ag_send, ag_recv, mt_send, mt_recv, xd_send, xd_recv, md_send, md_recv,
    zd_send, zd_recv, lf_send, lf_recv, rs_send, rs_recv,
):
    me = lax.axis_index(AXIS)
    chip, core = me // 2, lax.rem(me, 2)
    mate = chip * 2 + 1 - core
    next_chip = (lax.rem(chip + 1, n_chips), lax.rem(chip + n_chips - 1, n_chips))
    far = n_chips // 2
    last = 2 * far - 1
    _, n_exp, d_model, d_ff = w_in.shape
    n_tok = xbuf.shape[1] // 2
    quarter = n_tok // 4
    cap = leafbuf.shape[-2]
    wide = d_model // 4
    top_k = ids.shape[0]
    bf16, f32 = jnp.bfloat16, jnp.float32
    sends = chain_order(far)
    n_leaf = 4

    def rows(kind, part, side):
        return pl.ds(pl.multiple_of(kind * n_tok + part * 2 * quarter + side * quarter, quarter), quarter)

    def both_sides(kind, part):
        return pl.ds(pl.multiple_of(kind * n_tok + part * 2 * quarter, 2 * quarter), 2 * quarter)

    def krows(kind):
        return pl.ds(pl.multiple_of(kind * n_tok, n_tok), n_tok)

    def remote(src, dst, send, recv, to):
        return pltpu.make_async_remote_copy(
            src_ref=src, dst_ref=dst, send_sem=send, recv_sem=recv, device_id={AXIS: to}, device_id_type=MESH
        )

    def ag_copy(step, way, part, src_i, src_side):
        return remote(
            xbuf.at[src_i, rows(core, part, src_side)], xbuf.at[step + 1, rows(core, part, way)],
            ag_send, ag_recv.at[step, part], next_chip[way] * 2 + core,
        )

    def mt_copy(hop, way):
        return remote(
            meta.at[hop, core, way], meta.at[hop + 1, core, way],
            mt_send, mt_recv.at[hop], next_chip[way] * 2 + core,
        )

    def xd_copy(i, kind):
        return remote(xbuf.at[i, krows(kind)], xbuf.at[i, krows(kind)], xd_send, xd_recv.at[i], mate)

    def md_copy(hop, kind):
        return remote(meta.at[hop, kind], meta.at[hop, kind], md_send, md_recv.at[hop], mate)

    def zd_copy(i):
        return remote(zbuf.at[i, krows(1 - core)], zpart.at[i], zd_send, zd_recv.at[i // last], mate)

    def group_of(length, way):
        order = (far, far - 1, far + 1, far - 2)
        return order.index(length if way == RIGHT else n_chips - 1 - length)

    def leaf_copy(n, way, kind):
        return remote(
            packbuf.at[n, way, kind], leafbuf.at[n, way, core], lf_send, lf_recv.at[n], next_chip[way] * 2 + kind
        )

    def rs_copy(n, way):
        return remote(
            sumbuf.at[n - n_leaf, way], recvbuf.at[n - n_leaf, way], rs_send, rs_recv.at[n - n_leaf], next_chip[way] * 2 + core
        )

    def drain(ref, sem):
        pltpu.make_async_copy(ref, ref, sem).wait()

    loads = [
        pltpu.make_async_copy(a, b, load_sem.at[j])
        for a, b, j in (
            (tok_hbm, xbuf.at[0, krows(core)], 0),
            (ids_hbm, ids, 1), (wts_hbm, wts, 1), (dslot_hbm, dslot, 1), (eslot_hbm, eslot, 1),
            (wg_hbm, w_in.at[0], 2), (wu_hbm, w_in.at[1], 2), (wd_hbm, wd, 3),
        )
    ]
    loads[0].start()
    barrier = pltpu.get_barrier_semaphore()
    pl.semaphore_signal(barrier, inc=1, device_id={AXIS: mate}, device_id_type=MESH)
    for way in (RIGHT, LEFT):
        for kind in (0, 1):
            pl.semaphore_signal(barrier, inc=1, device_id={AXIS: next_chip[way] * 2 + kind}, device_id_type=MESH)
    for load in loads[1:]:
        load.start()
    loads[0].wait()
    pl.semaphore_wait(barrier, 5)

    for part in (0, 1):
        for way in (RIGHT, LEFT):
            ag_copy(0, way, part, 0, way).start()
    drain(gate_col.at[0, : 4 * top_k], load_sem.at[1])
    kept = (dslot[...] >= 0) & (eslot[...] >= 0)
    expert = jnp.where(kept, ids[...], -1).astype(f32)
    table = jnp.concatenate([wts[...], expert], axis=0).astype(bf16)
    for way in (RIGHT, LEFT):
        meta[0, core, way] = table
    for way in (RIGHT, LEFT):
        mt_copy(0, way).start()
    for part in (0, 1):
        for way in (RIGHT, LEFT):
            ag_copy(1, way, part, 0, 1 - way).start()
    drain(w_in, load_sem.at[2])
    loads[7].wait()

    def experts_of(hop, kind, side):
        return meta[hop, kind, side].astype(f32)[top_k:]

    def routed(expert, device):
        hits = sum(
            jnp.sum((expert == (device * n_exp + e).astype(f32)).astype(f32), axis=0, keepdims=True) for e in range(n_exp)
        )
        return hits > 0.0

    def ranks(masks):
        lines = [m.astype(f32) for m in masks] + [jnp.zeros((8 - len(masks), n_tok), f32)]
        before = lax.broadcasted_iota(jnp.int32, (n_tok, n_tok), 0) < lax.broadcasted_iota(jnp.int32, (n_tok, n_tok), 1)
        return jnp.dot(jnp.concatenate(lines, axis=0).astype(bf16), before.astype(bf16), preferred_element_type=f32)

    def packer(mask, rank):
        place = lax.broadcasted_iota(jnp.int32, (cap, n_tok), 0).astype(f32)
        return jnp.where(mask & (place == rank), 1.0, 0.0)

    def place(ahead, way):
        if ahead in (0, far):
            return [(0 if ahead == 0 else last, part, side) for part in (0, 1) for side in (RIGHT, LEFT)]
        side, hop = (1 - way, ahead) if ahead < far else (way, n_chips - ahead)
        return [(2 * hop - 1 if side == h else 2 * hop, part, side) for part in (0, 1) for h in (0, 1)]

    def experts_ahead(ahead, way, kind):
        if ahead == far:
            return experts_of(far, kind, RIGHT)
        return experts_of(ahead, kind, 1 - way) if ahead < far else experts_of(n_chips - ahead, kind, way)

    def arrive(i, part):
        drain(xbuf.at[i, both_sides(core, part)], ag_recv.at[i - 1, part])

        @pl.when(i <= last - 2)
        def _():
            for way in (RIGHT, LEFT):
                ag_copy(i + 1, way, part, i, way).start()

        if part == 1:

            @pl.when(lax.rem(i, 2) == 1)
            def _():
                hop = (i + 1) // 2
                drain(meta.at[hop, core], mt_recv.at[hop - 1])

                @pl.when(hop < far)
                def _():
                    for way in (RIGHT, LEFT):
                        mt_copy(hop, way).start()

    def compute(i, kind):
        hop = (i + 1) // 2
        fresh = (lax.rem(i, 2) == 1) | (i == 0)

        @pl.when(fresh)
        def _():
            lines = []
            for side in (RIGHT, LEFT):
                both = meta[hop, kind, side].astype(f32)
                for e in range(n_exp):
                    mine = both[top_k:] == (me * n_exp + e).astype(f32)
                    lines.append(jnp.sum(jnp.where(mine, both[:top_k], 0.0), axis=0, keepdims=True))
            lines.append(jnp.zeros((8 - len(lines), n_tok), f32))
            gate_col[kind, :, :8] = jnp.concatenate(lines, axis=0).T

        x = xbuf[i, krows(kind)]
        blk = 256
        for e in range(n_exp):
            for b in range(d_ff // blk):
                cols = pl.ds(b * blk, blk)
                g = jnp.dot(x, w_in[0, e, :, cols], preferred_element_type=f32)
                u = jnp.dot(x, w_in[1, e, :, cols], preferred_element_type=f32)
                hid[e, :, cols] = (jax.nn.silu(g) * u).astype(bf16)
        gates = []
        for e in range(n_exp):
            parts = []
            for part in (0, 1):
                for side in (RIGHT, LEFT):
                    start = (part * 2 + jnp.where(fresh, side, 1 - side)) * quarter
                    col = side * n_exp + e
                    parts.append(gate_col[kind, pl.ds(pl.multiple_of(start, quarter), quarter), col : col + 1])
            gates.append(jnp.concatenate(parts, axis=0))
        for b in range(d_model // blk):
            cols = pl.ds(b * blk, blk)
            z = None
            for e in range(n_exp):
                y = jnp.dot(hid[e], wd[e, :, cols], preferred_element_type=f32)
                y = y.astype(bf16).astype(f32)
                term = jnp.where(gates[e] != 0.0, gates[e] * y, 0.0)
                z = term if z is None else z + term
            zbuf[i, krows(kind), cols] = z.astype(bf16)

    def prepare(ahead):
        pairs = [(kind, way) for kind in (0, 1) for way in ((RIGHT,) if ahead == far else (RIGHT, LEFT))]
        masks = [routed(experts_ahead(ahead, way, kind), me) for kind, way in pairs]
        rank = ranks(masks)
        for j, (kind, way) in enumerate(pairs):
            picks[kind, (ahead - far + 2) * 2 + way] = packer(masks[j], rank[j : j + 1]).astype(bf16)

    def send_leaves(pairs):
        packed = []
        for n, kind in pairs:
            length, _ = sends[n]
            for way in (RIGHT, LEFT):
                ahead, toward = (length, way) if length <= far else (n_chips - length, 1 - way)
                pick = picks[kind, (ahead - far + 2) * 2 + (RIGHT if ahead == far else toward)]
                cols = pl.ds(group_of(length, way) * wide, wide)
                z = jnp.concatenate([zbuf[i, rows(kind, part, side), cols] for i, part, side in place(length, way)], axis=0)
                packed.append((n, way, kind, jnp.dot(pick, z, preferred_element_type=f32)))
        for n, way, kind, z in packed:
            packbuf[n, way, kind] = z.astype(bf16)
        for n, way, kind, _ in packed:
            leaf_copy(n, way, kind).start()

    def fresh_hop(i, move):
        @pl.when((lax.rem(i, 2) == 1) | (i == 0))
        def _():
            move((i + 1) // 2)

    def step(turn, carry):
        i = turn // 2
        even = lax.rem(turn, 2) == 0

        @pl.when(even)
        def _():
            @pl.when(i >= 1)
            def _():
                arrive(i, 1)

            xd_copy(i, core).start()
            fresh_hop(i, lambda hop: md_copy(hop, core).start())

        @pl.when(jnp.logical_not(even))
        def _():
            @pl.when(i < last)
            def _():
                arrive(i + 1, 0)

            fresh_hop(i, lambda hop: md_copy(hop, 1 - core).wait_recv())

            @pl.when(i == last)
            def _():
                prepare(far)

            xd_copy(i, 1 - core).wait_recv()

        kind = jnp.where(even, core, 1 - core)
        compute(i, kind)

        @pl.when(jnp.logical_not(even))
        def _():
            zd_copy(i).start()

        @pl.when(turn == 2 * last - 7)
        def _():
            prepare(far - 2)

        @pl.when(turn == 2 * last - 4)
        def _():
            send_leaves([(0, 0), (0, 1)])

        @pl.when(turn == 2 * last - 3)
        def _():
            prepare(far - 1)

        @pl.when((turn == 2 * last - 2) | (turn == 2 * last - 1))
        def _():
            send_leaves([(1, kind), (2, kind)])

        @pl.when(turn == 2 * last + 1)
        def _():
            send_leaves([(3, 0), (3, 1)])

        return carry

    lax.fori_loop(0, 2 * last + 2, step, 0)

    def unpack(n, way):
        ahead = sends[n][0] - 1
        expert = experts_ahead(ahead, way, core)
        masks = [routed(expert, next_chip[1 - way] * 2 + k) for k in (0, 1)]
        rank = ranks(masks)
        spread = [packer(masks[k], rank[k : k + 1]).T.astype(bf16) for k in (0, 1)]
        if way == RIGHT:
            drain(leafbuf.at[n], lf_recv.at[n])
        return sum(jnp.dot(spread[k], leafbuf[n, way, k], preferred_element_type=f32) for k in (0, 1))

    def own_part(ahead, way, cols):
        parts = [
            zbuf[i, rows(core, part, side), cols].astype(f32) + zpart[i, rows(0, part, side), cols].astype(f32)
            for i, part, side in place(ahead, way)
        ]
        return jnp.concatenate(parts, axis=0)

    drain(zpart.at[:last], zd_recv.at[0])
    for n in range(n_leaf, len(sends)):
        length, ahead = sends[n]
        src = sends.index((length, ahead + 1))
        if ahead == far:
            drain(zpart.at[last], zd_recv.at[1])
        for way in (RIGHT, LEFT):
            own = own_part(ahead, way, pl.ds(group_of(length, way) * wide, wide))
            if src < n_leaf:
                came = unpack(src, way)
            else:
                if way == RIGHT:
                    drain(recvbuf.at[src - n_leaf], rs_recv.at[src - n_leaf])
                came = recvbuf[src - n_leaf, way]
            sumbuf[n - n_leaf, way] = came + own
            rs_copy(n, way).start()

    ends = [n for n in range(len(sends)) if sends[n][1] == 1]
    known = set()
    for n in ends[2:]:
        for way in (RIGHT, LEFT):
            length = sends[n][0]
            group = group_of(length, way)
            other = sends.index((n_chips - 1 - length, 1))
            cols = pl.ds(group * wide, wide)
            own = own_part(0, way, cols)
            for m in (other, n):
                if m not in known:
                    known.add(m)
                    drain(recvbuf.at[m - n_leaf], rs_recv.at[m - n_leaf])
            came = recvbuf[n - n_leaf, way] + recvbuf[other - n_leaf, 1 - way]
            out_ref[:, cols] = (came + own).astype(out_ref.dtype)

    drain(xbuf.at[1:, :n_tok], ag_send)
    drain(meta.at[:far, 0], mt_send)
    drain(xbuf.at[:, :n_tok], xd_send)
    drain(meta.at[:, 0], md_send)
    drain(zpart, zd_send)
    drain(packbuf, lf_send)
    drain(sumbuf, rs_send)


def solution(mesh):
    groups = mesh.shape[AXIS]
    n_chips = groups // 2
    far = n_chips // 2
    last = 2 * far - 1
    n_sums = len(chain_order(far)) - 4
    row_spec = P(("data", "expert"), None)
    weight_spec = P("expert", None, None)

    def device_layer(tokens, expert_ids, gate_wts, dev_slot, exp_slot, w_gate, w_up, w_down):
        tok_dev, top_k = expert_ids.shape
        d_model = tokens.shape[1]
        e_local, _, d_ff = w_gate.shape
        dev_cap = min(tok_dev, 8 * ((3 * tok_dev * top_k + 16 * groups - 1) // (16 * groups)))
        bf16, f32, i32 = jnp.bfloat16, jnp.float32, jnp.int32
        dma = pltpu.SemaphoreType.DMA
        args = (tokens, expert_ids.T, gate_wts.T, dev_slot.T, exp_slot.T, w_gate, w_up, w_down)
        args = [pltpu.with_memory_space_constraint(a, pltpu.HBM) for a in args]
        return pl.pallas_call(
            functools.partial(moe_kernel, n_chips),
            out_shape=jax.ShapeDtypeStruct((tok_dev, d_model), bf16),
            in_specs=[pl.BlockSpec(memory_space=pltpu.HBM)] * len(args),
            out_specs=pl.BlockSpec(memory_space=pltpu.VMEM),
            scratch_shapes=[
                pltpu.VMEM((last + 1, 2 * tok_dev, d_model), bf16),
                pltpu.VMEM((last + 1, 2 * tok_dev, d_model), bf16),
                pltpu.VMEM((last + 1, tok_dev, d_model), bf16),
                pltpu.VMEM((4, 2, 2, dev_cap, d_model // 4), bf16),
                pltpu.VMEM((4, 2, 2, dev_cap, d_model // 4), bf16),
                pltpu.VMEM((n_sums, 2, tok_dev, d_model // 4), f32),
                pltpu.VMEM((n_sums, 2, tok_dev, d_model // 4), f32),
                pltpu.VMEM((far + 1, 2, 2, 2 * top_k, tok_dev), bf16),
                pltpu.VMEM((2, tok_dev, 128), f32),
                pltpu.VMEM((2, 5, dev_cap, tok_dev), bf16),
                pltpu.VMEM((e_local, tok_dev, d_ff), bf16),
                pltpu.VMEM((2, *w_gate.shape), bf16),
                pltpu.VMEM(w_down.shape, bf16),
                pltpu.VMEM((top_k, tok_dev), i32),
                pltpu.VMEM((top_k, tok_dev), f32),
                pltpu.VMEM((top_k, tok_dev), i32),
                pltpu.VMEM((top_k, tok_dev), i32),
                dma((4,)),
                dma, dma((last, 2)),
                dma, dma((far,)),
                dma, dma((last + 1,)),
                dma, dma((far + 1,)),
                dma, dma((2,)),
                dma, dma((4,)),
                dma, dma((n_sums,)),
            ],
            compiler_params=pltpu.CompilerParams(
                collective_id=0, has_side_effects=True, vmem_limit_bytes=48 * 1024 * 1024
            ),
        )(*args)

    def moe_layer(tokens, expert_ids, gate_wts, dev_slot, exp_slot, w_gate, w_up, w_down):
        mapped = jax.shard_map(device_layer, mesh=mesh, in_specs=(row_spec,) * 5 + (weight_spec,) * 3, out_specs=row_spec, check_vma=False)
        return mapped(tokens, expert_ids, gate_wts, dev_slot, exp_slot, w_gate, w_up, w_down)

    return moe_layer
```

```python
import functools

import jax
import jax.numpy as jnp
from jax import lax
from jax.experimental import pallas as pl
from jax.experimental.pallas import tpu as pltpu
from jax.sharding import PartitionSpec as P

MESH = pl.DeviceIdType.MESH
AXIS = "expert"
RIGHT, LEFT = 0, 1


def chain_order(far):
    a, b, c, d = far + 2, far - 1, far, far - 3
    assert d == 1
    return [
        (a, 6), (d, 1), (b, 3), (c, 4), (a, 5), (b, 2), (a, 4), (c, 3), (b, 1), (a, 3), (c, 2), (a, 2), (c, 1), (a, 1),
    ]


def moe_kernel(
    n_chips,
    tok_hbm, ids_hbm, wts_hbm, dslot_hbm, eslot_hbm, wg_hbm, wu_hbm, wd_hbm,
    out_ref,
    xbuf, zbuf, zpart, packbuf, leafbuf, sumbuf, recvbuf, meta, gate_col, picks, direct, hid, w_in, wd, ids, wts, dslot, eslot,
    load_sem, ag_send, ag_recv, mt_send, mt_recv, xd_send, xd_recv, md_send, md_recv,
    zd_send, zd_recv, lf_send, lf_recv, rs_send, rs_recv,
):
    me = lax.axis_index(AXIS)
    chip, core = me // 2, lax.rem(me, 2)
    mate = chip * 2 + 1 - core
    next_chip = (lax.rem(chip + 1, n_chips), lax.rem(chip + n_chips - 1, n_chips))
    far = n_chips // 2
    last = 2 * far - 1
    _, n_exp, d_model, d_ff = w_in.shape
    n_tok = xbuf.shape[1] // 2
    quarter = n_tok // 4
    cap = leafbuf.shape[-2]
    wide = d_model // 4
    top_k = ids.shape[0]
    bf16, f32 = jnp.bfloat16, jnp.float32
    sends = chain_order(far)
    n_leaf = 4

    def rows(kind, part, side):
        return pl.ds(pl.multiple_of(kind * n_tok + part * 2 * quarter + side * quarter, quarter), quarter)

    def both_sides(kind, part):
        return pl.ds(pl.multiple_of(kind * n_tok + part * 2 * quarter, 2 * quarter), 2 * quarter)

    def krows(kind):
        return pl.ds(pl.multiple_of(kind * n_tok, n_tok), n_tok)

    def remote(src, dst, send, recv, to):
        return pltpu.make_async_remote_copy(
            src_ref=src, dst_ref=dst, send_sem=send, recv_sem=recv, device_id={AXIS: to}, device_id_type=MESH
        )

    def ag_copy(step, way, part, src_i, src_side):
        return remote(
            xbuf.at[src_i, rows(core, part, src_side)], xbuf.at[step + 1, rows(core, part, way)],
            ag_send, ag_recv.at[step, part], next_chip[way] * 2 + core,
        )

    def mt_copy(hop, way):
        return remote(
            meta.at[hop, core, way], meta.at[hop + 1, core, way],
            mt_send, mt_recv.at[hop], next_chip[way] * 2 + core,
        )

    def xd_copy(i, kind):
        return remote(xbuf.at[i, krows(kind)], xbuf.at[i, krows(kind)], xd_send, xd_recv.at[i], mate)

    def md_copy(hop, kind):
        return remote(meta.at[hop, kind], meta.at[hop, kind], md_send, md_recv.at[hop], mate)

    def zd_copy(i):
        return remote(zbuf.at[i, krows(1 - core)], zpart.at[i], zd_send, zd_recv.at[i // last], mate)

    def group_of(length, way):
        order = (far, far - 1, far + 2, far - 3)
        return order.index(length if way == RIGHT else n_chips - 1 - length)

    def leaf_copy(n, way, kind):
        return remote(
            packbuf.at[n, way, kind], leafbuf.at[n, way, core], lf_send, lf_recv.at[n], next_chip[way] * 2 + kind
        )

    def rs_copy(n, way):
        return remote(
            sumbuf.at[n - n_leaf, way], recvbuf.at[n - n_leaf, way], rs_send, rs_recv.at[n - n_leaf], next_chip[way] * 2 + core
        )

    def drain(ref, sem):
        pltpu.make_async_copy(ref, ref, sem).wait()

    loads = [
        pltpu.make_async_copy(a, b, load_sem.at[j])
        for a, b, j in (
            (tok_hbm, xbuf.at[0, krows(core)], 0),
            (ids_hbm, ids, 1), (wts_hbm, wts, 1), (dslot_hbm, dslot, 1), (eslot_hbm, eslot, 1),
            (wg_hbm, w_in.at[0], 2), (wu_hbm, w_in.at[1], 2), (wd_hbm, wd, 3),
        )
    ]
    loads[0].start()
    barrier = pltpu.get_barrier_semaphore()
    pl.semaphore_signal(barrier, inc=1, device_id={AXIS: mate}, device_id_type=MESH)
    for way in (RIGHT, LEFT):
        for kind in (0, 1):
            pl.semaphore_signal(barrier, inc=1, device_id={AXIS: next_chip[way] * 2 + kind}, device_id_type=MESH)
    for load in loads[1:]:
        load.start()
    loads[0].wait()
    pl.semaphore_wait(barrier, 5)

    for part in (0, 1):
        for way in (RIGHT, LEFT):
            ag_copy(0, way, part, 0, way).start()
    drain(gate_col.at[0, : 4 * top_k], load_sem.at[1])
    kept = (dslot[...] >= 0) & (eslot[...] >= 0)
    expert = jnp.where(kept, ids[...], -1).astype(f32)
    table = jnp.concatenate([wts[...], expert], axis=0).astype(bf16)
    for way in (RIGHT, LEFT):
        meta[0, core, way] = table
    for way in (RIGHT, LEFT):
        mt_copy(0, way).start()
    for part in (0, 1):
        for way in (RIGHT, LEFT):
            ag_copy(1, way, part, 0, 1 - way).start()
    drain(w_in, load_sem.at[2])
    loads[7].wait()

    def experts_of(hop, kind, side):
        return meta[hop, kind, side].astype(f32)[top_k:]

    def routed(expert, device):
        hits = sum(
            jnp.sum((expert == (device * n_exp + e).astype(f32)).astype(f32), axis=0, keepdims=True) for e in range(n_exp)
        )
        return hits > 0.0

    def ranks(masks):
        lines = [m.astype(f32) for m in masks] + [jnp.zeros((8 - len(masks), n_tok), f32)]
        before = lax.broadcasted_iota(jnp.int32, (n_tok, n_tok), 0) < lax.broadcasted_iota(jnp.int32, (n_tok, n_tok), 1)
        return jnp.dot(jnp.concatenate(lines, axis=0).astype(bf16), before.astype(bf16), preferred_element_type=f32)

    def packer(mask, rank):
        place = lax.broadcasted_iota(jnp.int32, (cap, n_tok), 0).astype(f32)
        return jnp.where(mask & (place == rank), 1.0, 0.0)

    def place(ahead, way):
        if ahead in (0, far):
            return [(0 if ahead == 0 else last, part, side) for part in (0, 1) for side in (RIGHT, LEFT)]
        side, hop = (1 - way, ahead) if ahead < far else (way, n_chips - ahead)
        return [(2 * hop - 1 if side == h else 2 * hop, part, side) for part in (0, 1) for h in (0, 1)]

    def experts_ahead(ahead, way, kind):
        if ahead == far:
            return experts_of(far, kind, RIGHT)
        return experts_of(ahead, kind, 1 - way) if ahead < far else experts_of(n_chips - ahead, kind, way)

    def arrive(i, part):
        drain(xbuf.at[i, both_sides(core, part)], ag_recv.at[i - 1, part])

        @pl.when(i <= last - 2)
        def _():
            for way in (RIGHT, LEFT):
                ag_copy(i + 1, way, part, i, way).start()

        if part == 1:

            @pl.when(lax.rem(i, 2) == 1)
            def _():
                hop = (i + 1) // 2
                drain(meta.at[hop, core], mt_recv.at[hop - 1])

                @pl.when(hop < far)
                def _():
                    for way in (RIGHT, LEFT):
                        mt_copy(hop, way).start()

    def compute(i, kind):
        hop = (i + 1) // 2
        fresh = (lax.rem(i, 2) == 1) | (i == 0)

        @pl.when(fresh)
        def _():
            lines = []
            for side in (RIGHT, LEFT):
                both = meta[hop, kind, side].astype(f32)
                for e in range(n_exp):
                    mine = both[top_k:] == (me * n_exp + e).astype(f32)
                    lines.append(jnp.sum(jnp.where(mine, both[:top_k], 0.0), axis=0, keepdims=True))
            lines.append(jnp.zeros((8 - len(lines), n_tok), f32))
            gate_col[kind, :, :8] = jnp.concatenate(lines, axis=0).T

        x = xbuf[i, krows(kind)]
        blk = 256
        for e in range(n_exp):
            for b in range(d_ff // blk):
                cols = pl.ds(b * blk, blk)
                g = jnp.dot(x, w_in[0, e, :, cols], preferred_element_type=f32)
                u = jnp.dot(x, w_in[1, e, :, cols], preferred_element_type=f32)
                hid[e, :, cols] = (jax.nn.silu(g) * u).astype(bf16)
        gates = []
        for e in range(n_exp):
            parts = []
            for part in (0, 1):
                for side in (RIGHT, LEFT):
                    start = (part * 2 + jnp.where(fresh, side, 1 - side)) * quarter
                    col = side * n_exp + e
                    parts.append(gate_col[kind, pl.ds(pl.multiple_of(start, quarter), quarter), col : col + 1])
            gates.append(jnp.concatenate(parts, axis=0))
        for b in range(d_model // blk):
            cols = pl.ds(b * blk, blk)
            z = None
            for e in range(n_exp):
                y = jnp.dot(hid[e], wd[e, :, cols], preferred_element_type=f32)
                y = y.astype(bf16).astype(f32)
                term = jnp.where(gates[e] != 0.0, gates[e] * y, 0.0)
                z = term if z is None else z + term
            zbuf[i, krows(kind), cols] = z.astype(bf16)

    def prepare(ahead):
        pairs = [(kind, way) for kind in (0, 1) for way in ((RIGHT,) if ahead == far else (RIGHT, LEFT))]
        masks = [routed(experts_ahead(ahead, way, kind), me) for kind, way in pairs]
        rank = ranks(masks)
        for j, (kind, way) in enumerate(pairs):
            picks[kind, (ahead - 1) * 2 + way] = packer(masks[j], rank[j : j + 1]).astype(bf16)

    def send_leaves(pairs):
        packed = []
        for n, kind in pairs:
            length, _ = sends[n]
            for way in (RIGHT, LEFT):
                ahead, toward = (length, way) if length <= far else (n_chips - length, 1 - way)
                pick = picks[kind, (ahead - 1) * 2 + (RIGHT if ahead == far else toward)]
                cols = pl.ds(group_of(length, way) * wide, wide)
                z = jnp.concatenate([zbuf[i, rows(kind, part, side), cols] for i, part, side in place(length, way)], axis=0)
                packed.append((n, way, kind, jnp.dot(pick, z, preferred_element_type=f32)))
        for n, way, kind, z in packed:
            packbuf[n, way, kind] = z.astype(bf16)
        for n, way, kind, _ in packed:
            leaf_copy(n, way, kind).start()

    def unpack(n, way):
        ahead = sends[n][0] - 1
        expert = experts_ahead(ahead, way, core)
        masks = [routed(expert, next_chip[1 - way] * 2 + k) for k in (0, 1)]
        rank = ranks(masks)
        spread = [packer(masks[k], rank[k : k + 1]).T.astype(bf16) for k in (0, 1)]
        if way == RIGHT:
            drain(leafbuf.at[n], lf_recv.at[n])
        return sum(jnp.dot(spread[k], leafbuf[n, way, k], preferred_element_type=f32) for k in (0, 1))

    def own_part(ahead, way, cols):
        parts = [
            zbuf[i, rows(core, part, side), cols].astype(f32) + zpart[i, rows(0, part, side), cols].astype(f32)
            for i, part, side in place(ahead, way)
        ]
        return jnp.concatenate(parts, axis=0)

    def back(n):
        length, ahead = sends[n]
        src = sends.index((length, ahead + 1))
        if ahead == far:
            drain(zpart.at[last], zd_recv.at[1])
        for way in (RIGHT, LEFT):
            own = own_part(ahead, way, pl.ds(group_of(length, way) * wide, wide))
            if src < n_leaf:
                came = unpack(src, way)
            else:
                if way == RIGHT:
                    drain(recvbuf.at[src - n_leaf], rs_recv.at[src - n_leaf])
                came = recvbuf[src - n_leaf, way]
            sumbuf[n - n_leaf, way] = came + own
            rs_copy(n, way).start()

    def fresh_hop(i, move):
        @pl.when((lax.rem(i, 2) == 1) | (i == 0))
        def _():
            move((i + 1) // 2)

    def step(turn, carry):
        i = turn // 2
        even = lax.rem(turn, 2) == 0

        @pl.when(even)
        def _():
            @pl.when(i >= 1)
            def _():
                arrive(i, 1)

            xd_copy(i, core).start()
            fresh_hop(i, lambda hop: md_copy(hop, core).start())

        @pl.when(jnp.logical_not(even))
        def _():
            @pl.when(i < last)
            def _():
                arrive(i + 1, 0)

            fresh_hop(i, lambda hop: md_copy(hop, 1 - core).wait_recv())

            @pl.when(i == last)
            def _():
                prepare(far)

            xd_copy(i, 1 - core).wait_recv()

        kind = jnp.where(even, core, 1 - core)
        compute(i, kind)

        @pl.when(jnp.logical_not(even))
        def _():
            zd_copy(i).start()

        @pl.when(turn == 2 * last - 7)
        def _():
            prepare(far - 3)
            prepare(far - 2)

        @pl.when(turn == 2 * last - 4)
        def _():
            send_leaves([(0, 0), (0, 1)])
            send_leaves([(1, 0), (1, 1)])

        @pl.when(turn == 2 * last - 3)
        def _():
            prepare(far - 1)

        @pl.when((turn == 2 * last - 2) | (turn == 2 * last - 1))
        def _():
            send_leaves([(2, kind)])

        @pl.when(turn == 2 * last + 1)
        def _():
            send_leaves([(3, 0), (3, 1)])

        return carry

    lax.fori_loop(0, 2 * last + 2, step, 0)

    drain(zpart.at[:last], zd_recv.at[0])
    for n in range(n_leaf, len(sends)):
        back(n)
        if n == n_leaf + 2:
            for way in (RIGHT, LEFT):
                direct[way] = unpack(1, way)

    ends = [n for n in range(len(sends)) if sends[n][1] == 1]
    known = set()
    for n in ends[-2:]:
        for way in (RIGHT, LEFT):
            length = sends[n][0]
            group = group_of(length, way)
            other = sends.index((n_chips - 1 - length, 1))
            cols = pl.ds(group * wide, wide)
            own = own_part(0, way, cols)
            for m in (other, n):
                if m >= n_leaf and m not in known:
                    known.add(m)
                    drain(recvbuf.at[m - n_leaf], rs_recv.at[m - n_leaf])
            came = recvbuf[n - n_leaf, way] + (direct[1 - way] if other < n_leaf else recvbuf[other - n_leaf, 1 - way])
            out_ref[:, cols] = (came + own).astype(out_ref.dtype)

    drain(xbuf.at[1:, :n_tok], ag_send)
    drain(meta.at[:far, 0], mt_send)
    drain(xbuf.at[:, :n_tok], xd_send)
    drain(meta.at[:, 0], md_send)
    drain(zpart, zd_send)
    drain(packbuf, lf_send)
    drain(sumbuf, rs_send)


def solution(mesh):
    groups = mesh.shape[AXIS]
    n_chips = groups // 2
    far = n_chips // 2
    last = 2 * far - 1
    n_sums = len(chain_order(far)) - 4
    row_spec = P(("data", "expert"), None)
    weight_spec = P("expert", None, None)

    def device_layer(tokens, expert_ids, gate_wts, dev_slot, exp_slot, w_gate, w_up, w_down):
        tok_dev, top_k = expert_ids.shape
        d_model = tokens.shape[1]
        e_local, _, d_ff = w_gate.shape
        dev_cap = min(tok_dev, 8 * ((3 * tok_dev * top_k + 16 * groups - 1) // (16 * groups)))
        bf16, f32, i32 = jnp.bfloat16, jnp.float32, jnp.int32
        dma = pltpu.SemaphoreType.DMA
        args = (tokens, expert_ids.T, gate_wts.T, dev_slot.T, exp_slot.T, w_gate, w_up, w_down)
        args = [pltpu.with_memory_space_constraint(a, pltpu.HBM) for a in args]
        return pl.pallas_call(
            functools.partial(moe_kernel, n_chips),
            out_shape=jax.ShapeDtypeStruct((tok_dev, d_model), bf16),
            in_specs=[pl.BlockSpec(memory_space=pltpu.HBM)] * len(args),
            out_specs=pl.BlockSpec(memory_space=pltpu.VMEM),
            scratch_shapes=[
                pltpu.VMEM((last + 1, 2 * tok_dev, d_model), bf16),
                pltpu.VMEM((last + 1, 2 * tok_dev, d_model), bf16),
                pltpu.VMEM((last + 1, tok_dev, d_model), bf16),
                pltpu.VMEM((4, 2, 2, dev_cap, d_model // 4), bf16),
                pltpu.VMEM((4, 2, 2, dev_cap, d_model // 4), bf16),
                pltpu.VMEM((n_sums, 2, tok_dev, d_model // 4), f32),
                pltpu.VMEM((n_sums, 2, tok_dev, d_model // 4), f32),
                pltpu.VMEM((far + 1, 2, 2, 2 * top_k, tok_dev), bf16),
                pltpu.VMEM((2, tok_dev, 128), f32),
                pltpu.VMEM((2, last, dev_cap, tok_dev), bf16),
                pltpu.VMEM((2, tok_dev, d_model // 4), f32),
                pltpu.VMEM((e_local, tok_dev, d_ff), bf16),
                pltpu.VMEM((2, *w_gate.shape), bf16),
                pltpu.VMEM(w_down.shape, bf16),
                pltpu.VMEM((top_k, tok_dev), i32),
                pltpu.VMEM((top_k, tok_dev), f32),
                pltpu.VMEM((top_k, tok_dev), i32),
                pltpu.VMEM((top_k, tok_dev), i32),
                dma((4,)),
                dma, dma((last, 2)),
                dma, dma((far,)),
                dma, dma((last + 1,)),
                dma, dma((far + 1,)),
                dma, dma((2,)),
                dma, dma((4,)),
                dma, dma((n_sums,)),
            ],
            compiler_params=pltpu.CompilerParams(
                collective_id=0, has_side_effects=True, vmem_limit_bytes=48 * 1024 * 1024
            ),
        )(*args)

    def moe_layer(tokens, expert_ids, gate_wts, dev_slot, exp_slot, w_gate, w_up, w_down):
        mapped = jax.shard_map(device_layer, mesh=mesh, in_specs=(row_spec,) * 5 + (weight_spec,) * 3, out_specs=row_spec, check_vma=False)
        return mapped(tokens, expert_ids, gate_wts, dev_slot, exp_slot, w_gate, w_up, w_down)

    return moe_layer
```

```python
import functools

import jax
import jax.numpy as jnp
from jax import lax
from jax.experimental import pallas as pl
from jax.experimental.pallas import tpu as pltpu
from jax.sharding import PartitionSpec as P

MESH = pl.DeviceIdType.MESH
AXIS = "expert"
RIGHT, LEFT = 0, 1


def chain_order(far):
    a, b, c, d = far + 2, far - 1, far, far - 3
    assert d == 1
    return [
        (a, 6), (d, 1), (b, 3), (c, 4), (a, 5), (b, 2), (a, 4), (c, 3), (b, 1), (a, 3), (c, 2), (a, 2), (c, 1), (a, 1),
    ]


def moe_kernel(
    n_chips,
    tok_hbm, ids_hbm, wts_hbm, dslot_hbm, eslot_hbm, wg_hbm, wu_hbm, wd_hbm,
    out_ref,
    xbuf, zbuf, zpart, packbuf, leafbuf, sumbuf, recvbuf, meta, gate_col, picks, direct, hid, w_in, wd, ids, wts, dslot, eslot,
    load_sem, ag_send, ag_recv, mt_send, mt_recv, xd_send, xd_recv, md_send, md_recv,
    zd_send, zd_recv, lf_send, lf_recv, rs_send, rs_recv,
):
    me = lax.axis_index(AXIS)
    chip, core = me // 2, lax.rem(me, 2)
    mate = chip * 2 + 1 - core
    next_chip = (lax.rem(chip + 1, n_chips), lax.rem(chip + n_chips - 1, n_chips))
    far = n_chips // 2
    last = 2 * far - 1
    _, n_exp, d_model, d_ff = w_in.shape
    n_tok = xbuf.shape[1] // 2
    quarter = n_tok // 4
    cap = leafbuf.shape[-2]
    wide = d_model // 4
    top_k = ids.shape[0]
    bf16, f32 = jnp.bfloat16, jnp.float32
    sends = chain_order(far)
    n_leaf = 4

    def rows(kind, part, side):
        return pl.ds(pl.multiple_of(kind * n_tok + part * 2 * quarter + side * quarter, quarter), quarter)

    def both_sides(kind, part):
        return pl.ds(pl.multiple_of(kind * n_tok + part * 2 * quarter, 2 * quarter), 2 * quarter)

    def krows(kind):
        return pl.ds(pl.multiple_of(kind * n_tok, n_tok), n_tok)

    def remote(src, dst, send, recv, to):
        return pltpu.make_async_remote_copy(
            src_ref=src, dst_ref=dst, send_sem=send, recv_sem=recv, device_id={AXIS: to}, device_id_type=MESH
        )

    def ag_copy(step, way, part, src_i, src_side):
        return remote(
            xbuf.at[src_i, rows(core, part, src_side)], xbuf.at[step + 1, rows(core, part, way)],
            ag_send, ag_recv.at[step, part], next_chip[way] * 2 + core,
        )

    def mt_copy(hop, way):
        return remote(
            meta.at[hop, core, way], meta.at[hop + 1, core, way],
            mt_send, mt_recv.at[hop], next_chip[way] * 2 + core,
        )

    def xd_copy(i, kind):
        return remote(xbuf.at[i, krows(kind)], xbuf.at[i, krows(kind)], xd_send, xd_recv.at[i], mate)

    def md_copy(hop, kind):
        return remote(meta.at[hop, kind], meta.at[hop, kind], md_send, md_recv.at[hop], mate)

    def zd_copy(i):
        return remote(zbuf.at[i, krows(1 - core)], zpart.at[i], zd_send, zd_recv.at[i // last], mate)

    def group_of(length, way):
        order = (far, far - 1, far + 2, far - 3)
        return order.index(length if way == RIGHT else n_chips - 1 - length)

    def leaf_copy(n, way, kind):
        return remote(
            packbuf.at[n, way, kind], leafbuf.at[n, way, core], lf_send, lf_recv.at[n], next_chip[way] * 2 + kind
        )

    def rs_copy(n, way):
        return remote(
            sumbuf.at[n - n_leaf, way], recvbuf.at[n - n_leaf, way], rs_send, rs_recv.at[n - n_leaf], next_chip[way] * 2 + core
        )

    def drain(ref, sem):
        pltpu.make_async_copy(ref, ref, sem).wait()

    loads = [
        pltpu.make_async_copy(a, b, load_sem.at[j])
        for a, b, j in (
            (tok_hbm, xbuf.at[0, krows(core)], 0),
            (ids_hbm, ids, 1), (wts_hbm, wts, 1), (dslot_hbm, dslot, 1), (eslot_hbm, eslot, 1),
            (wg_hbm, w_in.at[0], 2), (wu_hbm, w_in.at[1], 2), (wd_hbm, wd, 3),
        )
    ]
    loads[0].start()
    barrier = pltpu.get_barrier_semaphore()
    pl.semaphore_signal(barrier, inc=1, device_id={AXIS: mate}, device_id_type=MESH)
    for way in (RIGHT, LEFT):
        for kind in (0, 1):
            pl.semaphore_signal(barrier, inc=1, device_id={AXIS: next_chip[way] * 2 + kind}, device_id_type=MESH)
    for load in loads[1:]:
        load.start()
    loads[0].wait()
    pl.semaphore_wait(barrier, 5)

    for part in (0, 1):
        for way in (RIGHT, LEFT):
            ag_copy(0, way, part, 0, way).start()
    drain(gate_col.at[0, : 4 * top_k], load_sem.at[1])
    kept = (dslot[...] >= 0) & (eslot[...] >= 0)
    expert = jnp.where(kept, ids[...], -1).astype(f32)
    table = jnp.concatenate([wts[...], expert], axis=0).astype(bf16)
    for way in (RIGHT, LEFT):
        meta[0, core, way] = table
    for way in (RIGHT, LEFT):
        mt_copy(0, way).start()
    for part in (0, 1):
        for way in (RIGHT, LEFT):
            ag_copy(1, way, part, 0, 1 - way).start()
    drain(w_in, load_sem.at[2])
    loads[7].wait()

    def experts_of(hop, kind, side):
        return meta[hop, kind, side].astype(f32)[top_k:]

    def routed(expert, device):
        hits = sum(
            jnp.sum((expert == (device * n_exp + e).astype(f32)).astype(f32), axis=0, keepdims=True) for e in range(n_exp)
        )
        return hits > 0.0

    def ranks(masks):
        lines = [m.astype(f32) for m in masks] + [jnp.zeros((8 - len(masks), n_tok), f32)]
        before = lax.broadcasted_iota(jnp.int32, (n_tok, n_tok), 0) < lax.broadcasted_iota(jnp.int32, (n_tok, n_tok), 1)
        return jnp.dot(jnp.concatenate(lines, axis=0).astype(bf16), before.astype(bf16), preferred_element_type=f32)

    def packer(mask, rank):
        place = lax.broadcasted_iota(jnp.int32, (cap, n_tok), 0).astype(f32)
        return jnp.where(mask & (place == rank), 1.0, 0.0)

    def place(ahead, way):
        if ahead in (0, far):
            return [(0 if ahead == 0 else last, part, side) for part in (0, 1) for side in (RIGHT, LEFT)]
        side, hop = (1 - way, ahead) if ahead < far else (way, n_chips - ahead)
        return [(2 * hop - 1 if side == h else 2 * hop, part, side) for part in (0, 1) for h in (0, 1)]

    def experts_ahead(ahead, way, kind):
        if ahead == far:
            return experts_of(far, kind, RIGHT)
        return experts_of(ahead, kind, 1 - way) if ahead < far else experts_of(n_chips - ahead, kind, way)

    def arrive(i, part):
        drain(xbuf.at[i, both_sides(core, part)], ag_recv.at[i - 1, part])

        @pl.when(i <= last - 2)
        def _():
            for way in (RIGHT, LEFT):
                ag_copy(i + 1, way, part, i, way).start()

        if part == 1:

            @pl.when(lax.rem(i, 2) == 1)
            def _():
                hop = (i + 1) // 2
                drain(meta.at[hop, core], mt_recv.at[hop - 1])

                @pl.when(hop < far)
                def _():
                    for way in (RIGHT, LEFT):
                        mt_copy(hop, way).start()

    def compute(i, kind):
        hop = (i + 1) // 2
        fresh = (lax.rem(i, 2) == 1) | (i == 0)

        @pl.when(fresh)
        def _():
            lines = []
            for side in (RIGHT, LEFT):
                both = meta[hop, kind, side].astype(f32)
                for e in range(n_exp):
                    mine = both[top_k:] == (me * n_exp + e).astype(f32)
                    lines.append(jnp.sum(jnp.where(mine, both[:top_k], 0.0), axis=0, keepdims=True))
            lines.append(jnp.zeros((8 - len(lines), n_tok), f32))
            gate_col[kind, :, :8] = jnp.concatenate(lines, axis=0).T

        x = xbuf[i, krows(kind)]
        blk = 256
        for e in range(n_exp):
            for b in range(d_ff // blk):
                cols = pl.ds(b * blk, blk)
                g = jnp.dot(x, w_in[0, e, :, cols], preferred_element_type=f32)
                u = jnp.dot(x, w_in[1, e, :, cols], preferred_element_type=f32)
                hid[e, :, cols] = (jax.nn.silu(g) * u).astype(bf16)
        gates = []
        for e in range(n_exp):
            parts = []
            for part in (0, 1):
                for side in (RIGHT, LEFT):
                    start = (part * 2 + jnp.where(fresh, side, 1 - side)) * quarter
                    col = side * n_exp + e
                    parts.append(gate_col[kind, pl.ds(pl.multiple_of(start, quarter), quarter), col : col + 1])
            gates.append(jnp.concatenate(parts, axis=0))
        for b in range(d_model // blk):
            cols = pl.ds(b * blk, blk)
            z = None
            for e in range(n_exp):
                y = jnp.dot(hid[e], wd[e, :, cols], preferred_element_type=f32)
                y = y.astype(bf16).astype(f32)
                term = jnp.where(gates[e] != 0.0, gates[e] * y, 0.0)
                z = term if z is None else z + term
            zbuf[i, krows(kind), cols] = z.astype(bf16)

    def prepare(ahead):
        pairs = [(kind, way) for kind in (0, 1) for way in ((RIGHT,) if ahead == far else (RIGHT, LEFT))]
        masks = [routed(experts_ahead(ahead, way, kind), me) for kind, way in pairs]
        rank = ranks(masks)
        for j, (kind, way) in enumerate(pairs):
            picks[kind, (ahead - 1) * 2 + way] = packer(masks[j], rank[j : j + 1]).astype(bf16)

    def send_leaves(pairs):
        packed = []
        for n, kind in pairs:
            length, _ = sends[n]
            for way in (RIGHT, LEFT):
                ahead, toward = (length, way) if length <= far else (n_chips - length, 1 - way)
                pick = picks[kind, (ahead - 1) * 2 + (RIGHT if ahead == far else toward)]
                cols = pl.ds(group_of(length, way) * wide, wide)
                z = jnp.concatenate([zbuf[i, rows(kind, part, side), cols] for i, part, side in place(length, way)], axis=0)
                packed.append((n, way, kind, jnp.dot(pick, z, preferred_element_type=f32)))
        for n, way, kind, z in packed:
            packbuf[n, way, kind] = z.astype(bf16)
        for n, way, kind, _ in packed:
            leaf_copy(n, way, kind).start()

    def unpack(n, way):
        ahead = sends[n][0] - 1
        expert = experts_ahead(ahead, way, core)
        masks = [routed(expert, next_chip[1 - way] * 2 + k) for k in (0, 1)]
        rank = ranks(masks)
        spread = [packer(masks[k], rank[k : k + 1]).T.astype(bf16) for k in (0, 1)]
        if way == RIGHT:
            drain(leafbuf.at[n], lf_recv.at[n])
        return sum(jnp.dot(spread[k], leafbuf[n, way, k], preferred_element_type=f32) for k in (0, 1))

    def own_part(ahead, way, cols):
        parts = [
            zbuf[i, rows(core, part, side), cols].astype(f32) + zpart[i, rows(0, part, side), cols].astype(f32)
            for i, part, side in place(ahead, way)
        ]
        return jnp.concatenate(parts, axis=0)

    def back(n):
        length, ahead = sends[n]
        src = sends.index((length, ahead + 1))
        if ahead == far:
            drain(zpart.at[last], zd_recv.at[1])
        for way in (RIGHT, LEFT):
            own = own_part(ahead, way, pl.ds(group_of(length, way) * wide, wide))
            if src < n_leaf:
                came = unpack(src, way)
            else:
                if way == RIGHT:
                    drain(recvbuf.at[src - n_leaf], rs_recv.at[src - n_leaf])
                came = recvbuf[src - n_leaf, way]
            sumbuf[n - n_leaf, way] = came + own
            rs_copy(n, way).start()

    def fresh_hop(i, move):
        @pl.when((lax.rem(i, 2) == 1) | (i == 0))
        def _():
            move((i + 1) // 2)

    def step(turn, carry):
        i = turn // 2
        even = lax.rem(turn, 2) == 0

        @pl.when(even)
        def _():
            @pl.when(i >= 1)
            def _():
                arrive(i, 1)

            xd_copy(i, core).start()
            fresh_hop(i, lambda hop: md_copy(hop, core).start())

        @pl.when(jnp.logical_not(even))
        def _():
            @pl.when(i < last)
            def _():
                arrive(i + 1, 0)

            fresh_hop(i, lambda hop: md_copy(hop, 1 - core).wait_recv())

            @pl.when(i == last)
            def _():
                prepare(far)
                send_leaves([(3, core)])

            xd_copy(i, 1 - core).wait_recv()

        kind = jnp.where(even, core, 1 - core)
        compute(i, kind)

        @pl.when(jnp.logical_not(even))
        def _():
            zd_copy(i).start()

        @pl.when(turn == 2 * last - 7)
        def _():
            prepare(far - 3)
            prepare(far - 2)

        @pl.when(turn == 2 * last - 4)
        def _():
            send_leaves([(0, 0), (0, 1)])
            send_leaves([(1, 0), (1, 1)])

        @pl.when(turn == 2 * last - 3)
        def _():
            prepare(far - 1)

        @pl.when((turn == 2 * last - 2) | (turn == 2 * last - 1))
        def _():
            send_leaves([(2, kind)])

        @pl.when(turn == 2 * last + 1)
        def _():
            send_leaves([(3, 1 - core)])

        return carry

    lax.fori_loop(0, 2 * last + 2, step, 0)

    drain(zpart.at[:last], zd_recv.at[0])
    for n in range(n_leaf, len(sends)):
        back(n)
        if n == n_leaf + 2:
            for way in (RIGHT, LEFT):
                direct[way] = unpack(1, way)

    ends = [n for n in range(len(sends)) if sends[n][1] == 1]
    known = set()
    for n in ends[-2:]:
        for way in (RIGHT, LEFT):
            length = sends[n][0]
            group = group_of(length, way)
            other = sends.index((n_chips - 1 - length, 1))
            cols = pl.ds(group * wide, wide)
            own = own_part(0, way, cols)
            for m in (other, n):
                if m >= n_leaf and m not in known:
                    known.add(m)
                    drain(recvbuf.at[m - n_leaf], rs_recv.at[m - n_leaf])
            came = recvbuf[n - n_leaf, way] + (direct[1 - way] if other < n_leaf else recvbuf[other - n_leaf, 1 - way])
            out_ref[:, cols] = (came + own).astype(out_ref.dtype)

    drain(xbuf.at[1:, :n_tok], ag_send)
    drain(meta.at[:far, 0], mt_send)
    drain(xbuf.at[:, :n_tok], xd_send)
    drain(meta.at[:, 0], md_send)
    drain(zpart, zd_send)
    drain(packbuf, lf_send)
    drain(sumbuf, rs_send)


def solution(mesh):
    groups = mesh.shape[AXIS]
    n_chips = groups // 2
    far = n_chips // 2
    last = 2 * far - 1
    n_sums = len(chain_order(far)) - 4
    row_spec = P(("data", "expert"), None)
    weight_spec = P("expert", None, None)

    def device_layer(tokens, expert_ids, gate_wts, dev_slot, exp_slot, w_gate, w_up, w_down):
        tok_dev, top_k = expert_ids.shape
        d_model = tokens.shape[1]
        e_local, _, d_ff = w_gate.shape
        dev_cap = min(tok_dev, 8 * ((3 * tok_dev * top_k + 16 * groups - 1) // (16 * groups)))
        bf16, f32, i32 = jnp.bfloat16, jnp.float32, jnp.int32
        dma = pltpu.SemaphoreType.DMA
        args = (tokens, expert_ids.T, gate_wts.T, dev_slot.T, exp_slot.T, w_gate, w_up, w_down)
        args = [pltpu.with_memory_space_constraint(a, pltpu.HBM) for a in args]
        return pl.pallas_call(
            functools.partial(moe_kernel, n_chips),
            out_shape=jax.ShapeDtypeStruct((tok_dev, d_model), bf16),
            in_specs=[pl.BlockSpec(memory_space=pltpu.HBM)] * len(args),
            out_specs=pl.BlockSpec(memory_space=pltpu.VMEM),
            scratch_shapes=[
                pltpu.VMEM((last + 1, 2 * tok_dev, d_model), bf16),
                pltpu.VMEM((last + 1, 2 * tok_dev, d_model), bf16),
                pltpu.VMEM((last + 1, tok_dev, d_model), bf16),
                pltpu.VMEM((4, 2, 2, dev_cap, d_model // 4), bf16),
                pltpu.VMEM((4, 2, 2, dev_cap, d_model // 4), bf16),
                pltpu.VMEM((n_sums, 2, tok_dev, d_model // 4), f32),
                pltpu.VMEM((n_sums, 2, tok_dev, d_model // 4), f32),
                pltpu.VMEM((far + 1, 2, 2, 2 * top_k, tok_dev), bf16),
                pltpu.VMEM((2, tok_dev, 128), f32),
                pltpu.VMEM((2, last, dev_cap, tok_dev), bf16),
                pltpu.VMEM((2, tok_dev, d_model // 4), f32),
                pltpu.VMEM((e_local, tok_dev, d_ff), bf16),
                pltpu.VMEM((2, *w_gate.shape), bf16),
                pltpu.VMEM(w_down.shape, bf16),
                pltpu.VMEM((top_k, tok_dev), i32),
                pltpu.VMEM((top_k, tok_dev), f32),
                pltpu.VMEM((top_k, tok_dev), i32),
                pltpu.VMEM((top_k, tok_dev), i32),
                dma((4,)),
                dma, dma((last, 2)),
                dma, dma((far,)),
                dma, dma((last + 1,)),
                dma, dma((far + 1,)),
                dma, dma((2,)),
                dma, dma((4,)),
                dma, dma((n_sums,)),
            ],
            compiler_params=pltpu.CompilerParams(
                collective_id=0, has_side_effects=True, vmem_limit_bytes=48 * 1024 * 1024
            ),
        )(*args)

    def moe_layer(tokens, expert_ids, gate_wts, dev_slot, exp_slot, w_gate, w_up, w_down):
        mapped = jax.shard_map(device_layer, mesh=mesh, in_specs=(row_spec,) * 5 + (weight_spec,) * 3, out_specs=row_spec, check_vma=False)
        return mapped(tokens, expert_ids, gate_wts, dev_slot, exp_slot, w_gate, w_up, w_down)

    return moe_layer
```

```python
import functools

import jax
import jax.numpy as jnp
from jax import lax
from jax.experimental import pallas as pl
from jax.experimental.pallas import tpu as pltpu
from jax.sharding import PartitionSpec as P

MESH = pl.DeviceIdType.MESH
AXIS = "expert"
RIGHT, LEFT = 0, 1


def chain_order(far):
    a, b, c, d = far + 2, far - 1, far, far - 3
    assert d == 1
    return [
        (a, 6), (d, 1), (b, 3), (c, 4), (a, 5), (b, 2), (a, 4), (c, 3), (b, 1), (a, 3), (c, 2), (a, 2), (c, 1), (a, 1),
    ]


def moe_kernel(
    n_chips,
    tok_hbm, ids_hbm, wts_hbm, dslot_hbm, eslot_hbm, wg_hbm, wu_hbm, wd_hbm,
    out_ref,
    xbuf, zbuf, zpart, packbuf, leafbuf, sumbuf, recvbuf, meta, gate_col, picks, direct, hid, w_in, wd, ids, wts, dslot, eslot,
    load_sem, ag_send, ag_recv, mt_send, mt_recv, xd_send, xd_recv, md_send, md_recv,
    zd_send, zd_recv, lf_send, lf_recv, rs_send, rs_recv,
):
    me = lax.axis_index(AXIS)
    chip, core = me // 2, lax.rem(me, 2)
    mate = chip * 2 + 1 - core
    next_chip = (lax.rem(chip + 1, n_chips), lax.rem(chip + n_chips - 1, n_chips))
    far = n_chips // 2
    last = 2 * far - 1
    _, n_exp, d_model, d_ff = w_in.shape
    n_tok = xbuf.shape[1] // 2
    quarter = n_tok // 4
    cap = leafbuf.shape[-2]
    wide = d_model // 4
    top_k = ids.shape[0]
    bf16, f32 = jnp.bfloat16, jnp.float32
    sends = chain_order(far)
    n_leaf = 4

    def rows(kind, part, side):
        return pl.ds(pl.multiple_of(kind * n_tok + part * 2 * quarter + side * quarter, quarter), quarter)

    def both_sides(kind, part):
        return pl.ds(pl.multiple_of(kind * n_tok + part * 2 * quarter, 2 * quarter), 2 * quarter)

    def krows(kind):
        return pl.ds(pl.multiple_of(kind * n_tok, n_tok), n_tok)

    def remote(src, dst, send, recv, to):
        return pltpu.make_async_remote_copy(
            src_ref=src, dst_ref=dst, send_sem=send, recv_sem=recv, device_id={AXIS: to}, device_id_type=MESH
        )

    def ag_copy(step, way, part, src_i, src_side):
        return remote(
            xbuf.at[src_i, rows(core, part, src_side)], xbuf.at[step + 1, rows(core, part, way)],
            ag_send, ag_recv.at[step % 4, part], next_chip[way] * 2 + core,
        )

    def mt_copy(hop, way):
        return remote(
            meta.at[hop, core, way], meta.at[hop + 1, core, way],
            mt_send, mt_recv.at[hop], next_chip[way] * 2 + core,
        )

    def xd_copy(i, kind):
        return remote(xbuf.at[i, krows(kind)], xbuf.at[i, krows(kind)], xd_send, xd_recv.at[lax.rem(i, 2)], mate)

    def md_copy(hop, kind):
        return remote(meta.at[hop, kind], meta.at[hop, kind], md_send, md_recv.at[hop], mate)

    def zd_copy(i):
        return remote(zbuf.at[i, krows(1 - core)], zpart.at[i], zd_send, zd_recv.at[i // last], mate)

    def group_of(length, way):
        order = (far, far - 1, far + 2, far - 3)
        return order.index(length if way == RIGHT else n_chips - 1 - length)

    def leaf_copy(n, way, kind):
        return remote(
            packbuf.at[n, way, kind], leafbuf.at[n, way, core], lf_send, lf_recv.at[n], next_chip[way] * 2 + kind
        )

    def rs_copy(n, way):
        return remote(
            sumbuf.at[n - n_leaf, way], recvbuf.at[n - n_leaf, way], rs_send, rs_recv.at[n - n_leaf], next_chip[way] * 2 + core
        )

    def drain(ref, sem):
        pltpu.make_async_copy(ref, ref, sem).wait()

    loads = [
        pltpu.make_async_copy(a, b, load_sem.at[j])
        for a, b, j in (
            (tok_hbm, xbuf.at[0, krows(core)], 0),
            (ids_hbm, ids, 1), (wts_hbm, wts, 1), (dslot_hbm, dslot, 1), (eslot_hbm, eslot, 1),
            (wg_hbm, w_in.at[0], 2), (wu_hbm, w_in.at[1], 2), (wd_hbm, wd, 3),
        )
    ]
    loads[0].start()
    barrier = pltpu.get_barrier_semaphore()
    pl.semaphore_signal(barrier, inc=1, device_id={AXIS: mate}, device_id_type=MESH)
    for way in (RIGHT, LEFT):
        for kind in (0, 1):
            pl.semaphore_signal(barrier, inc=1, device_id={AXIS: next_chip[way] * 2 + kind}, device_id_type=MESH)
    for load in loads[1:]:
        load.start()
    loads[0].wait()
    pl.semaphore_wait(barrier, 5)

    for part in (0, 1):
        for way in (RIGHT, LEFT):
            ag_copy(0, way, part, 0, way).start()
    drain(gate_col.at[0, : 4 * top_k], load_sem.at[1])
    kept = (dslot[...] >= 0) & (eslot[...] >= 0)
    expert = jnp.where(kept, ids[...], -1).astype(f32)
    table = jnp.concatenate([wts[...], expert], axis=0).astype(bf16)
    for way in (RIGHT, LEFT):
        meta[0, core, way] = table
    for way in (RIGHT, LEFT):
        mt_copy(0, way).start()
    for part in (0, 1):
        for way in (RIGHT, LEFT):
            ag_copy(1, way, part, 0, 1 - way).start()
    drain(w_in, load_sem.at[2])
    loads[7].wait()

    def experts_of(hop, kind, side):
        return meta[hop, kind, side].astype(f32)[top_k:]

    def routed(expert, device):
        hits = sum(
            jnp.sum((expert == (device * n_exp + e).astype(f32)).astype(f32), axis=0, keepdims=True) for e in range(n_exp)
        )
        return hits > 0.0

    def ranks(masks):
        lines = [m.astype(f32) for m in masks] + [jnp.zeros((8 - len(masks), n_tok), f32)]
        before = lax.broadcasted_iota(jnp.int32, (n_tok, n_tok), 0) < lax.broadcasted_iota(jnp.int32, (n_tok, n_tok), 1)
        return jnp.dot(jnp.concatenate(lines, axis=0).astype(bf16), before.astype(bf16), preferred_element_type=f32)

    def packer(mask, rank):
        place = lax.broadcasted_iota(jnp.int32, (cap, n_tok), 0).astype(f32)
        return jnp.where(mask & (place == rank), 1.0, 0.0)

    def place(ahead, way):
        if ahead in (0, far):
            return [(0 if ahead == 0 else last, part, side) for part in (0, 1) for side in (RIGHT, LEFT)]
        side, hop = (1 - way, ahead) if ahead < far else (way, n_chips - ahead)
        return [(2 * hop - 1 if side == h else 2 * hop, part, side) for part in (0, 1) for h in (0, 1)]

    def experts_ahead(ahead, way, kind):
        if ahead == far:
            return experts_of(far, kind, RIGHT)
        return experts_of(ahead, kind, 1 - way) if ahead < far else experts_of(n_chips - ahead, kind, way)

    def arrive(i, part):
        drain(xbuf.at[i, both_sides(core, part)], ag_recv.at[lax.rem(i - 1, 4), part])

        @pl.when(i <= last - 2)
        def _():
            for way in (RIGHT, LEFT):
                ag_copy(i + 1, way, part, i, way).start()

        if part == 1:

            @pl.when(lax.rem(i, 2) == 1)
            def _():
                hop = (i + 1) // 2
                drain(meta.at[hop, core], mt_recv.at[hop - 1])

                @pl.when(hop < far)
                def _():
                    for way in (RIGHT, LEFT):
                        mt_copy(hop, way).start()

    def compute(i, kind):
        hop = (i + 1) // 2
        fresh = (lax.rem(i, 2) == 1) | (i == 0)

        @pl.when(fresh)
        def _():
            lines = []
            for side in (RIGHT, LEFT):
                both = meta[hop, kind, side].astype(f32)
                for e in range(n_exp):
                    mine = both[top_k:] == (me * n_exp + e).astype(f32)
                    lines.append(jnp.sum(jnp.where(mine, both[:top_k], 0.0), axis=0, keepdims=True))
            lines.append(jnp.zeros((8 - len(lines), n_tok), f32))
            gate_col[kind, :, :8] = jnp.concatenate(lines, axis=0).T

        x = xbuf[i, krows(kind)]
        blk = 256
        for e in range(n_exp):
            for b in range(d_ff // blk):
                cols = pl.ds(b * blk, blk)
                g = jnp.dot(x, w_in[0, e, :, cols], preferred_element_type=f32)
                u = jnp.dot(x, w_in[1, e, :, cols], preferred_element_type=f32)
                hid[e, :, cols] = (jax.nn.silu(g) * u).astype(bf16)
        gates = []
        for e in range(n_exp):
            parts = []
            for part in (0, 1):
                for side in (RIGHT, LEFT):
                    start = (part * 2 + jnp.where(fresh, side, 1 - side)) * quarter
                    col = side * n_exp + e
                    parts.append(gate_col[kind, pl.ds(pl.multiple_of(start, quarter), quarter), col : col + 1])
            gates.append(jnp.concatenate(parts, axis=0))
        for b in range(d_model // blk):
            cols = pl.ds(b * blk, blk)
            z = None
            for e in range(n_exp):
                y = jnp.dot(hid[e], wd[e, :, cols], preferred_element_type=f32)
                y = y.astype(bf16).astype(f32)
                term = jnp.where(gates[e] != 0.0, gates[e] * y, 0.0)
                z = term if z is None else z + term
            zbuf[i, krows(kind), cols] = z.astype(bf16)

    def prepare(ahead):
        pairs = [(kind, way) for kind in (0, 1) for way in ((RIGHT,) if ahead == far else (RIGHT, LEFT))]
        masks = [routed(experts_ahead(ahead, way, kind), me) for kind, way in pairs]
        rank = ranks(masks)
        for j, (kind, way) in enumerate(pairs):
            picks[kind, (ahead - 1) * 2 + way] = packer(masks[j], rank[j : j + 1]).astype(bf16)

    def send_leaves(pairs):
        packed = []
        for n, kind in pairs:
            length, _ = sends[n]
            for way in (RIGHT, LEFT):
                ahead, toward = (length, way) if length <= far else (n_chips - length, 1 - way)
                pick = picks[kind, (ahead - 1) * 2 + (RIGHT if ahead == far else toward)]
                cols = pl.ds(group_of(length, way) * wide, wide)
                z = jnp.concatenate([zbuf[i, rows(kind, part, side), cols] for i, part, side in place(length, way)], axis=0)
                packed.append((n, way, kind, jnp.dot(pick, z, preferred_element_type=f32)))
        for n, way, kind, z in packed:
            packbuf[n, way, kind] = z.astype(bf16)
        for n, way, kind, _ in packed:
            leaf_copy(n, way, kind).start()

    def unpack(n, way):
        ahead = sends[n][0] - 1
        expert = experts_ahead(ahead, way, core)
        masks = [routed(expert, next_chip[1 - way] * 2 + k) for k in (0, 1)]
        rank = ranks(masks)
        spread = [packer(masks[k], rank[k : k + 1]).T.astype(bf16) for k in (0, 1)]
        if way == RIGHT:
            drain(leafbuf.at[n], lf_recv.at[n])
        return sum(jnp.dot(spread[k], leafbuf[n, way, k], preferred_element_type=f32) for k in (0, 1))

    def own_part(ahead, way, cols):
        parts = [
            zbuf[i, rows(core, part, side), cols].astype(f32) + zpart[i, rows(0, part, side), cols].astype(f32)
            for i, part, side in place(ahead, way)
        ]
        return jnp.concatenate(parts, axis=0)

    def back(n):
        length, ahead = sends[n]
        src = sends.index((length, ahead + 1))
        if ahead == far:
            drain(zpart.at[last], zd_recv.at[1])
        for way in (RIGHT, LEFT):
            own = own_part(ahead, way, pl.ds(group_of(length, way) * wide, wide))
            if src < n_leaf:
                came = unpack(src, way)
            else:
                if way == RIGHT:
                    drain(recvbuf.at[src - n_leaf], rs_recv.at[src - n_leaf])
                came = recvbuf[src - n_leaf, way]
            sumbuf[n - n_leaf, way] = came + own
            rs_copy(n, way).start()

    def fresh_hop(i, move):
        @pl.when((lax.rem(i, 2) == 1) | (i == 0))
        def _():
            move((i + 1) // 2)

    def step(turn, carry):
        i = turn // 2
        even = lax.rem(turn, 2) == 0

        @pl.when(even)
        def _():
            @pl.when(i >= 1)
            def _():
                arrive(i, 1)

            xd_copy(i, core).start()
            fresh_hop(i, lambda hop: md_copy(hop, core).start())

        @pl.when(jnp.logical_not(even))
        def _():
            @pl.when(i < last)
            def _():
                arrive(i + 1, 0)

            fresh_hop(i, lambda hop: md_copy(hop, 1 - core).wait_recv())

            @pl.when(i == last)
            def _():
                prepare(far)
                send_leaves([(3, core)])

            xd_copy(i, 1 - core).wait_recv()

        kind = jnp.where(even, core, 1 - core)
        compute(i, kind)

        @pl.when(jnp.logical_not(even))
        def _():
            zd_copy(i).start()

        @pl.when(turn == 2 * last - 7)
        def _():
            prepare(far - 3)
            prepare(far - 2)

        @pl.when(turn == 2 * last - 4)
        def _():
            send_leaves([(0, 0), (0, 1)])
            send_leaves([(1, 0), (1, 1)])

        @pl.when(turn == 2 * last - 3)
        def _():
            prepare(far - 1)

        @pl.when((turn == 2 * last - 2) | (turn == 2 * last - 1))
        def _():
            send_leaves([(2, kind)])

        @pl.when(turn == 2 * last + 1)
        def _():
            send_leaves([(3, 1 - core)])

        return carry

    lax.fori_loop(0, 2 * last + 2, step, 0)

    drain(zpart.at[:last], zd_recv.at[0])
    for n in range(n_leaf, len(sends)):
        back(n)
        if n == n_leaf + 2:
            for way in (RIGHT, LEFT):
                direct[way] = unpack(1, way)

    ends = [n for n in range(len(sends)) if sends[n][1] == 1]
    known = set()
    for n in ends[-2:]:
        for way in (RIGHT, LEFT):
            length = sends[n][0]
            group = group_of(length, way)
            other = sends.index((n_chips - 1 - length, 1))
            cols = pl.ds(group * wide, wide)
            own = own_part(0, way, cols)
            for m in (other, n):
                if m >= n_leaf and m not in known:
                    known.add(m)
                    drain(recvbuf.at[m - n_leaf], rs_recv.at[m - n_leaf])
            came = recvbuf[n - n_leaf, way] + (direct[1 - way] if other < n_leaf else recvbuf[other - n_leaf, 1 - way])
            out_ref[:, cols] = (came + own).astype(out_ref.dtype)

    drain(xbuf.at[1:, :n_tok], ag_send)
    drain(meta.at[:far, 0], mt_send)
    drain(xbuf.at[:, :n_tok], xd_send)
    drain(meta.at[:, 0], md_send)
    drain(zpart, zd_send)
    drain(packbuf, lf_send)
    drain(sumbuf, rs_send)


def solution(mesh):
    groups = mesh.shape[AXIS]
    n_chips = groups // 2
    far = n_chips // 2
    last = 2 * far - 1
    n_sums = len(chain_order(far)) - 4
    row_spec = P(("data", "expert"), None)
    weight_spec = P("expert", None, None)

    def device_layer(tokens, expert_ids, gate_wts, dev_slot, exp_slot, w_gate, w_up, w_down):
        tok_dev, top_k = expert_ids.shape
        d_model = tokens.shape[1]
        e_local, _, d_ff = w_gate.shape
        dev_cap = min(tok_dev, 8 * ((3 * tok_dev * top_k + 16 * groups - 1) // (16 * groups)))
        bf16, f32, i32 = jnp.bfloat16, jnp.float32, jnp.int32
        dma = pltpu.SemaphoreType.DMA
        args = (tokens, expert_ids.T, gate_wts.T, dev_slot.T, exp_slot.T, w_gate, w_up, w_down)
        args = [pltpu.with_memory_space_constraint(a, pltpu.HBM) for a in args]
        return pl.pallas_call(
            functools.partial(moe_kernel, n_chips),
            out_shape=jax.ShapeDtypeStruct((tok_dev, d_model), bf16),
            in_specs=[pl.BlockSpec(memory_space=pltpu.HBM)] * len(args),
            out_specs=pl.BlockSpec(memory_space=pltpu.VMEM),
            scratch_shapes=[
                pltpu.VMEM((last + 1, 2 * tok_dev, d_model), bf16),
                pltpu.VMEM((last + 1, 2 * tok_dev, d_model), bf16),
                pltpu.VMEM((last + 1, tok_dev, d_model), bf16),
                pltpu.VMEM((4, 2, 2, dev_cap, d_model // 4), bf16),
                pltpu.VMEM((4, 2, 2, dev_cap, d_model // 4), bf16),
                pltpu.VMEM((n_sums, 2, tok_dev, d_model // 4), f32),
                pltpu.VMEM((n_sums, 2, tok_dev, d_model // 4), f32),
                pltpu.VMEM((far + 1, 2, 2, 2 * top_k, tok_dev), bf16),
                pltpu.VMEM((2, tok_dev, 128), f32),
                pltpu.VMEM((2, last, dev_cap, tok_dev), bf16),
                pltpu.VMEM((2, tok_dev, d_model // 4), f32),
                pltpu.VMEM((e_local, tok_dev, d_ff), bf16),
                pltpu.VMEM((2, *w_gate.shape), bf16),
                pltpu.VMEM(w_down.shape, bf16),
                pltpu.VMEM((top_k, tok_dev), i32),
                pltpu.VMEM((top_k, tok_dev), f32),
                pltpu.VMEM((top_k, tok_dev), i32),
                pltpu.VMEM((top_k, tok_dev), i32),
                dma((4,)),
                dma, dma((4, 2)),
                dma, dma((far,)),
                dma, dma((2,)),
                dma, dma((far + 1,)),
                dma, dma((2,)),
                dma, dma((4,)),
                dma, dma((n_sums,)),
            ],
            compiler_params=pltpu.CompilerParams(
                collective_id=0, has_side_effects=True, vmem_limit_bytes=48 * 1024 * 1024
            ),
        )(*args)

    def moe_layer(tokens, expert_ids, gate_wts, dev_slot, exp_slot, w_gate, w_up, w_down):
        mapped = jax.shard_map(device_layer, mesh=mesh, in_specs=(row_spec,) * 5 + (weight_spec,) * 3, out_specs=row_spec, check_vma=False)
        return mapped(tokens, expert_ids, gate_wts, dev_slot, exp_slot, w_gate, w_up, w_down)

    return moe_layer
```
